32 devices in a mesh: gx: 4 (over z), gy: 4 (over x, core), ens: 2 (over y).
Axes of the slice: x: 2, y: 2, z: 4, core: 2. Of those that a mesh axis runs over, the one named last changes fastest.
Arguments:
- state: float32 [128, 64, 512], P('ens', 'gy', 'gx'), may hold values from -6 to 6
- u_vel: float32 [64, 512], P('gy', 'gx'), may hold values from -0.4 to 0.4
- v_vel: float32 [64, 512], P('gy', 'gx'), may hold values from -0.4 to 0.4
- land: int32 [64, 512], P('gy', 'gx'), may hold values 0 or 1
- forcing: float32 [8, 64, 512], P(None, 'gy', 'gx'), may hold values from -3 to 3
- member_mode: int32 [128], P('ens'), may hold values from 0 to 7
- theta: float32 [128, 4], P('ens'), may hold values from -1 to 1
- obs_index: int32 [4, 4, 128], P('gy', 'gx'), may hold values from 0 to 2047
- obs_values: float32 [4, 4, 128], P('gy', 'gx'), may hold values from -6 to 6
- obs_sigma: float32 [4, 4, 128], P('gy', 'gx'), may hold values from 0.5 to 4
Outputs:
- final_state: float32 [128, 64, 512], P('ens', 'gy', 'gx')
- new_theta: float32 [128, 4], P('ens')
The draws below stay inside these ranges and needn't reach their ends.
All inputs are finite; a program needn't handle non-finite values. No bound on the sum of `land` on one device may be relied on, other than what follows from the above.
Results may differ from the reference program's by a relative error of at most 0.0003.
Values sent between devices are 32-bit elements; how exact they have to be, the bound alone decides.
A program may use at most 64 MiB of HBM per device.

```python
import math
import jax
import jax.numpy as jnp
from jax import lax

M = 128
P_SIZE = 4
K = 8
CX = 128
CY = 16
OBS_T = 128
STEPS = 4
NX = 512
NY = 64
N_GX = 4
N_GY = 4


def plant(entries, own_key, least, top_value):
    extent = entries.shape
    place = [jax.random.randint(jax.random.fold_in(own_key, axis), (), 0, extent[axis]) for axis in range(len(extent))]
    entries = entries.at[tuple(place)].set(least)
    longest = extent.index(max(extent))
    place[longest] = (place[longest] + 1) % extent[longest]
    return entries.at[tuple(place)].set(top_value)


def block_scale(stream_key, extent, cuts, low, largest):
    def one(dim, blocks):
        draws = jax.random.uniform(jax.random.fold_in(jax.random.fold_in(stream_key, 6), dim), (blocks,), jnp.float32, low / len(cuts), largest / len(cuts))
        return jnp.repeat(jnp.exp(draws), extent[dim] // blocks).reshape((-1,) + (1,) * (len(extent) - dim - 1))

    level = one(*cuts[0])
    for cut in cuts[1:]:
        level = level * one(*cut)
    return level


def scatter_about(key, dims, width, bound, shards=(), kind=jnp.bfloat16):
    gain = block_scale(key, dims, shards, -0.22, 0.18) if shards else 1.0
    drawn = jax.random.normal(key, dims, jnp.float32) * width * gain
    return jnp.minimum(jnp.maximum(drawn, -bound), bound).astype(kind)


def setup_inputs(seed: int = 0) -> dict:
    streams_of = jax.random.split(jax.random.key(seed), 11)
    return {
        "state": scatter_about(streams_of[0], (M, NY, NX), 1.0, 6.0, ((0, 2), (1, 4), (2, 4)), jnp.float32),
        "u_vel": jnp.clip(jax.random.uniform(streams_of[1], (NY, NX), jnp.float32, -0.4, 0.4) * block_scale(streams_of[1], (NY, NX), ((0, 4), (1, 4)), -0.4, 0.0), -0.4, 0.4),
        "v_vel": jnp.clip(jax.random.uniform(streams_of[2], (NY, NX), jnp.float32, -0.4, 0.4) * block_scale(streams_of[2], (NY, NX), ((0, 4), (1, 4)), -0.4, 0.0), -0.4, 0.4),
        "land": plant((jax.random.randint(streams_of[3], (NY, NX), 0, 8) < 1).astype(jnp.int32), jax.random.fold_in(streams_of[3], 1), 0, 1),
        "forcing": scatter_about(streams_of[4], (K, NY, NX), 0.5, 3.0, ((1, 4), (2, 4)), jnp.float32),
        "member_mode": plant(jax.random.randint(streams_of[5], (M,), 0, K), jax.random.fold_in(streams_of[5], 1), 0, K - 1).astype(jnp.int32),
        "theta": jnp.clip(jax.random.uniform(streams_of[6], (M, P_SIZE), jnp.float32, -1.0, 1.0) * block_scale(streams_of[6], (M, P_SIZE), ((0, 2),), -0.4, 0.0), -1.0, 1.0),
        "obs_index": plant(jax.random.randint(streams_of[7], (N_GY, N_GX, OBS_T), 0, CY * CX), jax.random.fold_in(streams_of[7], 1), 0, (CY * CX) - 1).astype(jnp.int32),
        "obs_values": scatter_about(streams_of[8], (N_GY, N_GX, OBS_T), 1.0, 6.0, ((0, 4), (1, 4)), jnp.float32),
        "obs_sigma": jnp.clip(jnp.exp(math.log(4.0) - 2.0794415 * jax.random.uniform(streams_of[9], (N_GY, N_GX, OBS_T), jnp.float32) ** block_scale(streams_of[9], (N_GY, N_GX, OBS_T), ((0, 4), (1, 4)), -0.2, 0.2)), 0.5, 4.0),
    }


def laplace(field):
    upper = jnp.pad(field[1:], ((0, 1), (0, 0)))
    lower = jnp.pad(field[:-1], ((1, 0), (0, 0)))
    return upper + lower + jnp.roll(field, -1, 1) + jnp.roll(field, 1, 1) - 4.0 * field

def reference(state, u_vel, v_vel, land, forcing, member_mode, theta, obs_index, obs_values, obs_sigma):
    ocean = (1 - land).astype(jnp.float32)
    tile_rows = jnp.arange(N_GY, dtype=jnp.int32)[:, None, None] * CY
    tile_cols = jnp.arange(N_GX, dtype=jnp.int32)[None, :, None] * CX
    site_rows = (tile_rows + obs_index // CX).reshape(-1)
    site_cols = (tile_cols + obs_index % CX).reshape(-1)

    def advance(member_data):
        field, mode, params = member_data
        diffuse = 0.05 * (1.0 + 0.5 * jnp.tanh(params[0]))
        hyper = 0.005 * (1.0 + 0.5 * jnp.tanh(params[1]))
        damping = 0.05 * (1.0 + 0.5 * jnp.tanh(params[2]))
        forced = params[3] * forcing[mode]
        for step_index in range(STEPS):
            lap_field = laplace(field)
            biharm = laplace(lap_field)
            upper = jnp.pad(field[1:], ((0, 1), (0, 0)))
            lower = jnp.pad(field[:-1], ((1, 0), (0, 0)))
            grad_x = 0.5 * (jnp.roll(field, -1, 1) - jnp.roll(field, 1, 1))
            grad_y = 0.5 * (upper - lower)
            tend = diffuse * lap_field - hyper * biharm - damping * field + forced - (u_vel * grad_x + v_vel * grad_y)
            field = (field + tend) * ocean
        return (field, field[site_rows, site_cols])
    final_state, observed = lax.map(advance, (state, member_mode, theta))
    sigma = obs_sigma.reshape(-1)
    target = obs_values.reshape(-1)
    anomaly = (observed - jnp.mean(observed, 0)) / sigma
    misfit = (target - observed) / sigma
    gram = jnp.dot(anomaly.astype(jnp.float32), anomaly.T.astype(jnp.float32), preferred_element_type=jnp.float32, precision=lax.Precision.HIGHEST)
    cross = jnp.dot(anomaly.astype(jnp.float32), misfit.T.astype(jnp.float32), preferred_element_type=jnp.float32, precision=lax.Precision.HIGHEST)
    system = gram + (M - 1) * jnp.eye(M, dtype=jnp.float32)
    weights = jnp.linalg.solve(system, cross)
    spread = theta - jnp.mean(theta, 0)
    new_theta = theta + jnp.dot(weights.T.astype(jnp.float32), spread.astype(jnp.float32), preferred_element_type=jnp.float32, precision=lax.Precision.HIGHEST)
    return (final_state, new_theta)
```

```python
import functools
import jax
import jax.numpy as jnp
from jax import lax
from jax.experimental import pallas as pl
from jax.experimental.pallas import tpu as pltpu
from jax.sharding import PartitionSpec as P

STEPS = 4
DEPTH = 2 * STEPS
F32 = jnp.float32
VM = pltpu.VMEM
MESH = pl.DeviceIdType.MESH
HIGH = lax.Precision.HIGHEST


def vspec():
    return pl.BlockSpec(memory_space=pltpu.VMEM)


def halo_kernel(n_gx, n_gy, q_ref, f_ref, qt_ref, qb_ref, ft_ref, fb_ref, mid_ref, top_ref, bot_ref,
                pack, row_send, row_recv, gx_send, gx_recv, gy_send, gy_recv):
    gx, gy = lax.axis_index("gx"), lax.axis_index("gy")
    right, left = lax.rem(gx + 1, n_gx), lax.rem(gx + n_gx - 1, n_gx)
    has_up, has_down = gy > 0, gy < n_gy - 1
    up, down = jnp.maximum(gy - 1, 0), jnp.minimum(gy + 1, n_gy - 1)
    members, rows, cols = q_ref.shape
    fields = f_ref.shape[0]

    barrier = pltpu.get_barrier_semaphore()
    pl.semaphore_signal(barrier, inc=1, device_id={"gx": right}, device_id_type=MESH)
    pl.semaphore_signal(barrier, inc=1, device_id={"gx": left}, device_id_type=MESH)

    @pl.when(has_up)
    def _():
        pl.semaphore_signal(barrier, inc=1, device_id={"gy": up}, device_id_type=MESH)

    @pl.when(has_down)
    def _():
        pl.semaphore_signal(barrier, inc=1, device_id={"gy": down}, device_id_type=MESH)

    lane = lax.broadcasted_iota(jnp.int32, (8, cols), 1)

    def pack_from(ref, base):
        def body(g, carry):
            lo = jnp.zeros((8, cols), F32)
            hi = jnp.zeros((8, cols), F32)
            for r in range(rows):
                val = ref[pl.ds(g * 8, 8), r, :]
                mine = (lane // DEPTH) == r
                hi = jnp.where(mine, pltpu.roll(val, (r * DEPTH + DEPTH) % cols, 1), hi)
                lo = jnp.where(mine, pltpu.roll(val, (r * DEPTH) % cols, 1), lo)
            pack[0, pl.ds(base + g * 8, 8), :] = hi
            pack[1, pl.ds(base + g * 8, 8), :] = lo
            return carry
        lax.fori_loop(0, ref.shape[0] // 8, body, 0)

    pl.semaphore_wait(barrier, 2 + has_up.astype(jnp.int32) + has_down.astype(jnp.int32))

    def rdma(src, dst, send, recv, dev):
        return pltpu.make_async_remote_copy(src_ref=src, dst_ref=dst, send_sem=send, recv_sem=recv,
                                            device_id=dev, device_id_type=MESH)

    downs = [rdma(q_ref.at[:, rows - DEPTH:, :], qt_ref, row_send.at[0], row_recv.at[0], {"gy": down}),
             rdma(f_ref.at[:, rows - DEPTH:, :], ft_ref, row_send.at[1], row_recv.at[1], {"gy": down})]
    ups = [rdma(q_ref.at[:, :DEPTH, :], qb_ref, row_send.at[2], row_recv.at[2], {"gy": up}),
           rdma(f_ref.at[:, :DEPTH, :], fb_ref, row_send.at[3], row_recv.at[3], {"gy": up})]
    strip_down = rdma(mid_ref, top_ref, gy_send.at[0], gy_recv.at[0], {"gy": down})
    strip_up = rdma(mid_ref, bot_ref, gy_send.at[1], gy_recv.at[1], {"gy": up})

    @pl.when(has_down)
    def _():
        for c in downs:
            c.start()

    @pl.when(has_up)
    def _():
        for c in ups:
            c.start()

    pack_from(q_ref, 0)
    pack_from(f_ref, members)
    to_right = rdma(pack.at[0], mid_ref.at[0], gx_send.at[0], gx_recv.at[0], {"gx": right})
    to_left = rdma(pack.at[1], mid_ref.at[1], gx_send.at[1], gx_recv.at[1], {"gx": left})
    to_right.start()
    to_left.start()
    to_right.wait()
    to_left.wait()

    @pl.when(has_down)
    def _():
        strip_down.start()

    @pl.when(has_up)
    def _():
        strip_up.start()

    @pl.when(has_down)
    def _():
        for c in downs + [strip_down]:
            c.wait_send()
        for c in ups + [strip_up]:
            c.wait_recv()

    @pl.when(has_up)
    def _():
        for c in ups + [strip_up]:
            c.wait_send()
        for c in downs + [strip_down]:
            c.wait_recv()


def halo_exchange(mesh, state, fields):
    members, rows, cols = state.shape
    nf = fields.shape[0]
    total = members + nf
    sds = jax.ShapeDtypeStruct
    return pl.pallas_call(
        functools.partial(halo_kernel, mesh.shape["gx"], mesh.shape["gy"]),
        out_shape=[sds((members, DEPTH, cols), F32), sds((members, DEPTH, cols), F32),
                   sds((nf, DEPTH, cols), F32), sds((nf, DEPTH, cols), F32),
                   sds((2, total, cols), F32), sds((2, total, cols), F32), sds((2, total, cols), F32)],
        in_specs=[vspec()] * 2,
        out_specs=[vspec()] * 7,
        scratch_shapes=[VM((2, total, cols), F32)]
        + [pltpu.SemaphoreType.DMA((4,))] * 2
        + [pltpu.SemaphoreType.DMA((2,))] * 4,
        compiler_params=pltpu.CompilerParams(collective_id=0, has_side_effects=True),
        name="halo",
    )(state, fields)


def model_kernel(n_gy, rows, q_ref, qt_ref, qb_ref, mid_ref, top_ref, bot_ref,
                 f_ref, ft_ref, fb_ref, fmid_ref, ftop_ref, fbot_ref,
                 mode_ref, theta_ref, index_ref, out_ref, obs_ref, thp_ref,
                 Q, FO, FP, ST):
    g = pl.program_id(0)
    gy = lax.axis_index("gy")
    cols = 128
    has_up, has_down = gy > 0, gy < n_gy - 1
    n_rows = rows + 2 * DEPTH
    shape = (8, cols)
    lane = lax.broadcasted_iota(jnp.int32, shape, 1)
    sub = lax.broadcasted_iota(jnp.int32, shape, 0)
    zero = jnp.zeros(shape, F32)

    def inside(i):
        return has_up if i < DEPTH else (has_down if i >= DEPTH + rows else None)

    def masked(i, x):
        ok = inside(i)
        return x if ok is None else jnp.where(ok, x, 0.0)

    def row_pair(i, base, q, qt, qb, mid, top, bot, mbase):
        if i < DEPTH:
            a = qt[pl.ds(base * DEPTH + i, 8, stride=DEPTH), :]
            strip, k = top, rows - DEPTH + i
        elif i < DEPTH + rows:
            a = q[pl.ds(base * rows + i - DEPTH, 8, stride=rows), :]
            strip, k = mid, i - DEPTH
        else:
            a = qb[pl.ds(base * DEPTH + i - DEPTH - rows, 8, stride=DEPTH), :]
            strip, k = bot, i - DEPTH - rows
        lo = pltpu.roll(strip[0, mbase:mbase + 8, :], (cols - DEPTH - k * DEPTH) % cols, 1)
        hi = pltpu.roll(strip[1, mbase:mbase + 8, :], (cols - k * DEPTH) % cols, 1)
        b = jnp.where(lane < DEPTH, hi, jnp.where(lane >= cols - DEPTH, lo, 0.0))
        return masked(i, a), masked(i, b)

    @pl.when(g == 0)
    def _():
        for i in range(n_rows):
            pa, pb = row_pair(i, 0, f_ref, ft_ref, fb_ref, fmid_ref, ftop_ref, fbot_ref, 0)
            FP[i, 0] = pa
            FP[i, 1] = pb
            sa, sb = row_pair(i, 8, f_ref, ft_ref, fb_ref, fmid_ref, ftop_ref, fbot_ref, 8)
            for h, s in ((0, sa), (1, sb)):
                ST[0, i, h] = jnp.broadcast_to(0.5 * s[0:1], shape)
                ST[1, i, h] = jnp.broadcast_to(0.5 * s[1:2], shape)
                ST[2, i, h] = jnp.broadcast_to(s[2:3], shape)

    th = theta_ref[...]
    diffuse = jnp.broadcast_to(0.05 * (1.0 + 0.5 * jnp.tanh(th[:, 0:1])), shape)
    hyper = jnp.broadcast_to(0.005 * (1.0 + 0.5 * jnp.tanh(th[:, 1:2])), shape)
    keep = jnp.broadcast_to(1.0 - 0.05 * (1.0 + 0.5 * jnp.tanh(th[:, 2:3])), shape)
    gain = jnp.broadcast_to(th[:, 3:4], shape)
    thp = zero
    for k in range(th.shape[1]):
        thp = jnp.where(lane == k, th[:, k:k + 1], thp)
    thp_ref[...] = thp

    mode = jnp.zeros(shape, jnp.int32)
    for k in range(8):
        mode = jnp.where(sub == k, mode_ref[g * 8 + k], mode)

    for i in range(n_rows):
        a, b = row_pair(i, 0, q_ref, qt_ref, qb_ref, mid_ref, top_ref, bot_ref, 0)
        Q[0, i, 0] = a
        Q[0, i, 1] = b
        if 2 <= i < n_rows - 2:
            for h in range(2):
                FO[i, h] = gain * jnp.take_along_axis(FP[i, h], mode, axis=0, mode="promise_in_bounds")

    first, last = lane == 0, lane == cols - 1

    def neighbours(a, b):
        ap, bp = pltpu.roll(a, cols - 1, 1), pltpu.roll(b, cols - 1, 1)
        am, bm = pltpu.roll(a, 1, 1), pltpu.roll(b, 1, 1)
        return ((jnp.where(last, bp, ap), jnp.where(first, bm, am)),
                (jnp.where(last, ap, bp), jnp.where(first, am, bm)))

    for s in range(STEPS):
        src, dst = s % 2, (s + 1) % 2
        lo, hi = 2 * s, n_rows - 2 * s
        final = s == STEPS - 1
        q, lap, grad = {}, {}, {}

        def load(i):
            q[i] = (Q[src, i, 0], Q[src, i, 1])

        def make_lap(i):
            pair = neighbours(*q[i])
            both, gr = [], []
            for h in range(2):
                xp, xm = pair[h]
                v = (q[i + 1][h] + q[i - 1][h]) + (xp + xm) - 4.0 * q[i][h]
                both.append(masked(i, v))
                gr.append(xp - xm)
            lap[i], grad[i] = tuple(both), gr

        load(lo)
        load(lo + 1)
        for i in range(lo + 2, lo + 4):
            load(i)
            make_lap(i - 1)
        for i in range(lo + 2, hi - 2):
            load(i + 2) if i + 2 < hi else None
            make_lap(i + 1)
            pair = neighbours(*lap[i])
            for h in range(1 if final else 2):
                xp, xm = pair[h]
                bi = (lap[i + 1][h] + lap[i - 1][h]) + (xp + xm) - 4.0 * lap[i][h]
                adv = ST[0, i, h] * grad[i][h] + ST[1, i, h] * (q[i + 1][h] - q[i - 1][h])
                new = keep * q[i][h] + diffuse * lap[i][h] - hyper * bi + (FO[i, h] - adv)
                new = new * ST[2, i, h]
                if final:
                    out_ref[pl.ds(i - DEPTH, 8, stride=rows), :] = new
                else:
                    Q[dst, i, h] = new

    index = index_ref[0]
    col = jnp.bitwise_and(index, cols - 1)
    row = jnp.right_shift(index, cols.bit_length() - 1)
    hot = (lax.broadcasted_iota(jnp.int32, (cols, cols), 0) == col).astype(jnp.bfloat16)
    x = out_ref[...]
    x1 = x.astype(jnp.bfloat16)
    rem = x - x1.astype(F32)
    x2 = rem.astype(jnp.bfloat16)
    x3 = (rem - x2.astype(F32)).astype(jnp.bfloat16)
    dot = functools.partial(jnp.dot, preferred_element_type=F32)
    picked = dot(x1, hot) + (dot(x2, hot) + dot(x3, hot))
    row_id = lax.broadcasted_iota(jnp.int32, (8, rows, cols), 1)
    obs_ref[...] = jnp.sum(jnp.where(row_id == row[None], picked.reshape(8, rows, cols), 0.0), axis=1)


def run_model(mesh, state, fields, halos, member_mode, theta, obs_index):
    members, rows, cols = state.shape
    nf = fields.shape[0]
    qt, qb, ft, fb, mid, top, bot = halos
    n_rows = rows + 2 * DEPTH
    sds = jax.ShapeDtypeStruct
    by_group = lambda n: pl.BlockSpec((8 * n, cols), lambda g: (g, 0))
    strip = pl.BlockSpec((2, 8, cols), lambda g: (0, g, 0))
    fstrip = pl.BlockSpec((2, nf, cols), lambda g: (0, members // nf, 0))
    whole = lambda n: pl.BlockSpec((nf * n, cols), lambda g: (0, 0))
    out, obs, thp = pl.pallas_call(
        functools.partial(model_kernel, mesh.shape["gy"], rows),
        grid=(members // 8,),
        out_shape=[sds((members * rows, cols), F32), sds((members, cols), F32), sds((members, cols), F32)],
        in_specs=[by_group(rows), by_group(DEPTH), by_group(DEPTH), strip, strip, strip,
                  whole(rows), whole(DEPTH), whole(DEPTH), fstrip, fstrip, fstrip,
                  pl.BlockSpec(memory_space=pltpu.SMEM),
                  pl.BlockSpec((8, theta.shape[1]), lambda g: (g, 0)),
                  pl.BlockSpec((1, 1, obs_index.shape[-1]), lambda g: (0, 0, 0))],
        out_specs=[by_group(rows), pl.BlockSpec((8, cols), lambda g: (g, 0)),
                   pl.BlockSpec((8, cols), lambda g: (g, 0))],
        scratch_shapes=[VM((2, n_rows, 2, 8, cols), F32), VM((n_rows, 2, 8, cols), F32),
                        VM((n_rows, 2, 8, cols), F32), VM((3, n_rows, 2, 8, cols), F32)],
        name="model",
    )(state.reshape(members * rows, cols), qt.reshape(-1, cols), qb.reshape(-1, cols), mid, top, bot,
      fields.reshape(-1, cols), ft.reshape(-1, cols), fb.reshape(-1, cols), mid, top, bot,
      member_mode, theta, obs_index)
    return out.reshape(members, rows, cols), obs, thp


def sums_kernel(n_gx, n_gy, n_ens, reduce_here, obs_ref, thp_ref, val_ref, sig_ref, full_ref, th_ref,
                obs_all, part, rs, ens_send, ens_recv, rs_send, rs_recv, ag_send, ag_recv):
    gx, gy, ens = lax.axis_index("gx"), lax.axis_index("gy"), lax.axis_index("ens")
    members = obs_ref.shape[0]
    n = n_gx * n_gy
    me = gy * n_gx + gx
    peers = [lax.rem(me + o, n) for o in range(1, n)] if reduce_here else []
    where = [{"gx": lax.rem(p, n_gx), "gy": lax.div(p, n_gx)} for p in peers]
    others = [lax.rem(ens + o, n_ens) for o in range(1, n_ens)]

    barrier = pltpu.get_barrier_semaphore()
    for p in others:
        pl.semaphore_signal(barrier, inc=1, device_id={"ens": p}, device_id_type=MESH)
    for p in where:
        pl.semaphore_signal(barrier, inc=1, device_id=p, device_id_type=MESH)
    pl.semaphore_wait(barrier, len(others) + len(where))

    def rdma(src, dst, send, recv, dev):
        return pltpu.make_async_remote_copy(src_ref=src, dst_ref=dst, send_sem=send, recv_sem=recv,
                                            device_id=dev, device_id_type=MESH)

    mine = pl.ds(pl.multiple_of(ens * members, members), members)
    copies = []
    for k, p in enumerate(others):
        copies.append(rdma(obs_ref, obs_all.at[mine], ens_send.at[2 * k], ens_recv.at[2 * k], {"ens": p}))
        copies.append(rdma(thp_ref, th_ref.at[mine], ens_send.at[2 * k + 1], ens_recv.at[2 * k + 1], {"ens": p}))
    for c in copies:
        c.start()
    obs_all[mine, :] = obs_ref[...]
    th_ref[mine, :] = thp_ref[...]
    for c in copies:
        c.wait()

    x = obs_all[...]
    mean = jnp.mean(x, axis=0, keepdims=True)
    inv = 1.0 / sig_ref[0]
    anom = (x - mean) * inv
    d = jnp.broadcast_to((val_ref[0] - mean) * inv, x.shape)
    nt = (((1,), (1,)), ((), ()))
    total = x.shape[0]
    part[:, 0:total] = lax.dot_general(anom, anom, nt, preferred_element_type=F32, precision=HIGH)
    part[:, total:] = lax.dot_general(anom, d, nt, preferred_element_type=F32, precision=HIGH)

    if not reduce_here:
        full_ref[...] = part[...]
        return
    own = total // n
    at = lambda p: pl.ds(pl.multiple_of(p * own, own), own)
    sends = [rdma(part.at[at(p)], rs.at[k], rs_send.at[k], rs_recv.at[k], w)
             for k, (p, w) in enumerate(zip(peers, where))]
    for c in sends:
        c.start()
    acc = part[at(me), :]
    for k, c in enumerate(sends):
        c.wait_recv()
        acc = acc + rs[k]
    full_ref[at(me), :] = acc
    gathers = [rdma(full_ref.at[at(me)], full_ref.at[at(me)], ag_send.at[k], ag_recv.at[k], w)
               for k, w in enumerate(where)]
    for c in gathers:
        c.start()
    for c in sends:
        c.wait_send()
    for c in gathers:
        c.wait()


def ensemble_sums(mesh, obs, thp, values, sigma):
    n_gx, n_gy, n_ens = mesh.shape["gx"], mesh.shape["gy"], mesh.shape["ens"]
    members, cols = obs.shape
    total = members * n_ens
    n = n_gx * n_gy
    reduce_here = total % (8 * n) == 0
    own = total // n if reduce_here else 8
    slots = n - 1 if reduce_here else 1
    full, th = pl.pallas_call(
        functools.partial(sums_kernel, n_gx, n_gy, n_ens, reduce_here),
        out_shape=[jax.ShapeDtypeStruct((total, 2 * total), F32), jax.ShapeDtypeStruct((total, cols), F32)],
        in_specs=[vspec()] * 4,
        out_specs=[vspec()] * 2,
        scratch_shapes=[VM((total, cols), F32), VM((total, 2 * total), F32), VM((slots, own, 2 * total), F32)]
        + [pltpu.SemaphoreType.DMA((2 * (n_ens - 1),))] * 2
        + [pltpu.SemaphoreType.DMA((slots,))] * 4,
        compiler_params=pltpu.CompilerParams(collective_id=1, has_side_effects=True),
        name="sums",
    )(obs, thp, values, sigma)
    if not reduce_here:
        full = lax.psum(full, ("gx", "gy"))
    return full, th


def solve_kernel(members, full_ref, th_ref, out_ref, xs):
    total = full_ref.shape[0]
    blocks = total // 8
    shape = (8, total)
    lane = lax.broadcasted_iota(jnp.int32, shape, 1)
    sub = lax.broadcasted_iota(jnp.int32, shape, 0)
    th = th_ref[...]
    mean = jnp.mean(th, axis=0, keepdims=True)
    A, R = [], []
    for k in range(blocks):
        rows = slice(8 * k, 8 * k + 8)
        A.append(full_ref[rows, 0:total] + jnp.where(lane == sub + 8 * k, float(total - 1), 0.0))
        R.append(th[rows] - mean)
    for k in range(blocks):
        pa, pr = A[k], R[k]
        for j in range(8):
            c = pa[:, 8 * k + j:8 * k + j + 1]
            inv = 1.0 / c[j:j + 1]
            na, nr = pa[j:j + 1] * inv, pr[j:j + 1] * inv
            pa = jnp.where(sub == j, na, pa - c * na)
            pr = jnp.where(sub == j, nr, pr - c * nr)
        A[k], R[k] = pa, pr
        for i in list(range(k + 1, blocks)) + list(range(k)):
            a, r = A[i], R[i]
            for j in range(8):
                c = A[i][:, 8 * k + j:8 * k + j + 1]
                a = a - c * pa[j:j + 1]
                r = r - c * pr[j:j + 1]
            A[i], R[i] = a, r
    shift = jnp.zeros((1, th.shape[1]), F32)
    for k in range(blocks):
        rows = slice(8 * k, 8 * k + 8)
        shift = shift + jnp.sum(full_ref[rows, total:] * R[k], axis=0, keepdims=True)
        xs[rows, :] = R[k]
    ens = lax.axis_index("ens")
    x = xs[pl.ds(pl.multiple_of(ens * members, members), members), :]
    new = mean + shift + float(total - 1) * x
    out_ref[...] = new[:, 0:out_ref.shape[1]]


def solve(full, th, theta):
    return pl.pallas_call(
        functools.partial(solve_kernel, theta.shape[0]),
        out_shape=jax.ShapeDtypeStruct(theta.shape, F32),
        in_specs=[vspec()] * 2,
        out_specs=vspec(),
        scratch_shapes=[VM(th.shape, F32)],
        name="solve",
    )(full, th)


def local(mesh, state, u_vel, v_vel, land, forcing, member_mode, theta, obs_index, obs_values, obs_sigma):
    ocean = (1 - land).astype(F32)
    rows, cols = u_vel.shape
    fields = jnp.concatenate([forcing, u_vel[None], v_vel[None], ocean[None], jnp.zeros((5, rows, cols), F32)], 0)
    halos = halo_exchange(mesh, state, fields)
    final, obs, thp = run_model(mesh, state, fields, halos, member_mode, theta, obs_index)
    full, th = ensemble_sums(mesh, obs, thp, obs_values, obs_sigma)
    return final, solve(full, th, theta)


def solution(mesh):
    placed = (
        P("ens", "gy", "gx"),
        P("gy", "gx"),
        P("gy", "gx"),
        P("gy", "gx"),
        P(None, "gy", "gx"),
        P("ens"),
        P("ens", None),
        P("gy", "gx", None),
        P("gy", "gx", None),
        P("gy", "gx", None),
    )
    return jax.shard_map(
        functools.partial(local, mesh),
        mesh=mesh,
        in_specs=placed,
        out_specs=(P("ens", "gy", "gx"), P("ens", None)),
        check_vma=False,
    )
```

```python
import functools
import jax
import jax.numpy as jnp
from jax import lax
from jax.experimental import pallas as pl
from jax.experimental.pallas import tpu as pltpu
from jax.sharding import PartitionSpec as P

STEPS = 4
DEPTH = 2 * STEPS
F32 = jnp.float32
VM = pltpu.VMEM
MESH = pl.DeviceIdType.MESH
HIGH = lax.Precision.HIGHEST


def vspec():
    return pl.BlockSpec(memory_space=pltpu.VMEM)


def halo_kernel(n_gx, n_gy, q_ref, f_ref, qt_ref, qb_ref, ft_ref, fb_ref, mid_ref, top_ref, bot_ref,
                pack, row_send, row_recv, gx_send, gx_recv, gy_send, gy_recv):
    gx, gy = lax.axis_index("gx"), lax.axis_index("gy")
    right, left = lax.rem(gx + 1, n_gx), lax.rem(gx + n_gx - 1, n_gx)
    has_up, has_down = gy > 0, gy < n_gy - 1
    up, down = jnp.maximum(gy - 1, 0), jnp.minimum(gy + 1, n_gy - 1)
    members, rows, cols = q_ref.shape
    fields = f_ref.shape[0]

    barrier = pltpu.get_barrier_semaphore()
    pl.semaphore_signal(barrier, inc=1, device_id={"gx": right}, device_id_type=MESH)
    pl.semaphore_signal(barrier, inc=1, device_id={"gx": left}, device_id_type=MESH)

    @pl.when(has_up)
    def _():
        pl.semaphore_signal(barrier, inc=1, device_id={"gy": up}, device_id_type=MESH)

    @pl.when(has_down)
    def _():
        pl.semaphore_signal(barrier, inc=1, device_id={"gy": down}, device_id_type=MESH)

    lane = lax.broadcasted_iota(jnp.int32, (8, cols), 1)

    def pack_from(ref, base):
        def body(g, carry):
            lo = jnp.zeros((8, cols), F32)
            hi = jnp.zeros((8, cols), F32)
            for r in range(rows):
                val = ref[pl.ds(g * 8, 8), r, :]
                mine = (lane // DEPTH) == r
                hi = jnp.where(mine, pltpu.roll(val, (r * DEPTH + DEPTH) % cols, 1), hi)
                lo = jnp.where(mine, pltpu.roll(val, (r * DEPTH) % cols, 1), lo)
            pack[0, pl.ds(base + g * 8, 8), :] = hi
            pack[1, pl.ds(base + g * 8, 8), :] = lo
            return carry
        lax.fori_loop(0, ref.shape[0] // 8, body, 0)

    pl.semaphore_wait(barrier, 2 + has_up.astype(jnp.int32) + has_down.astype(jnp.int32))

    def rdma(src, dst, send, recv, dev):
        return pltpu.make_async_remote_copy(src_ref=src, dst_ref=dst, send_sem=send, recv_sem=recv,
                                            device_id=dev, device_id_type=MESH)

    downs = [rdma(q_ref.at[:, rows - DEPTH:, :], qt_ref, row_send.at[0], row_recv.at[0], {"gy": down}),
             rdma(f_ref.at[:, rows - DEPTH:, :], ft_ref, row_send.at[1], row_recv.at[1], {"gy": down})]
    ups = [rdma(q_ref.at[:, :DEPTH, :], qb_ref, row_send.at[2], row_recv.at[2], {"gy": up}),
           rdma(f_ref.at[:, :DEPTH, :], fb_ref, row_send.at[3], row_recv.at[3], {"gy": up})]
    strip_down = rdma(mid_ref, top_ref, gy_send.at[0], gy_recv.at[0], {"gy": down})
    strip_up = rdma(mid_ref, bot_ref, gy_send.at[1], gy_recv.at[1], {"gy": up})

    @pl.when(has_down)
    def _():
        for c in downs:
            c.start()

    @pl.when(has_up)
    def _():
        for c in ups:
            c.start()

    pack_from(q_ref, 0)
    pack_from(f_ref, members)
    to_right = rdma(pack.at[0], mid_ref.at[0], gx_send.at[0], gx_recv.at[0], {"gx": right})
    to_left = rdma(pack.at[1], mid_ref.at[1], gx_send.at[1], gx_recv.at[1], {"gx": left})
    to_right.start()
    to_left.start()
    to_right.wait()
    to_left.wait()

    @pl.when(has_down)
    def _():
        strip_down.start()

    @pl.when(has_up)
    def _():
        strip_up.start()

    @pl.when(has_down)
    def _():
        for c in downs + [strip_down]:
            c.wait_send()
        for c in ups + [strip_up]:
            c.wait_recv()

    @pl.when(has_up)
    def _():
        for c in ups + [strip_up]:
            c.wait_send()
        for c in downs + [strip_down]:
            c.wait_recv()


def halo_exchange(mesh, state, fields):
    members, rows, cols = state.shape
    nf = fields.shape[0]
    total = members + nf
    sds = jax.ShapeDtypeStruct
    return pl.pallas_call(
        functools.partial(halo_kernel, mesh.shape["gx"], mesh.shape["gy"]),
        out_shape=[sds((members, DEPTH, cols), F32), sds((members, DEPTH, cols), F32),
                   sds((nf, DEPTH, cols), F32), sds((nf, DEPTH, cols), F32),
                   sds((2, total, cols), F32), sds((2, total, cols), F32), sds((2, total, cols), F32)],
        in_specs=[vspec()] * 2,
        out_specs=[vspec()] * 7,
        scratch_shapes=[VM((2, total, cols), F32)]
        + [pltpu.SemaphoreType.DMA((4,))] * 2
        + [pltpu.SemaphoreType.DMA((2,))] * 4,
        compiler_params=pltpu.CompilerParams(collective_id=0, has_side_effects=True),
        name="halo",
    )(state, fields)


def model_kernel(n_gy, q_ref, qt_ref, qb_ref, f_ref, ft_ref, fb_ref, mid_ref, top_ref, bot_ref,
                 mode_ref, theta_ref, index_ref, out_ref, obs_ref, thp_ref,
                 Q, L, FO, US, H, LH, FH, UH, TH):
    gy = lax.axis_index("gy")
    members = mode_ref.shape[1]
    cols = q_ref.shape[1]
    rows = q_ref.shape[0] // members
    n_rows = rows + 2 * DEPTH
    has_up, has_down = gy > 0, gy < n_gy - 1
    shape = (8, cols)
    lane = lax.broadcasted_iota(jnp.int32, shape, 1)
    sub = lax.broadcasted_iota(jnp.int32, shape, 0)
    half_ok = jnp.where(lane < cols // 2, has_down.astype(jnp.int32), has_up.astype(jnp.int32)) > 0
    bits = {k: jnp.bitwise_and(lane, k) != 0 for k in (1, 2, 4)}

    def roll(x, k):
        return pltpu.roll(x, k % cols, 1)

    def butterfly(xs):
        xs = list(xs)
        for k in (1, 2, 4):
            for v in range(8):
                if not v & k:
                    x, y = xs[v], xs[v | k]
                    xs[v] = jnp.where(bits[k], roll(y, k), x)
                    xs[v | k] = jnp.where(bits[k], y, roll(x, -k))
        return xs

    def masked(i, x):
        if i < DEPTH:
            return jnp.where(has_up, x, 0.0)
        if i >= DEPTH + rows:
            return jnp.where(has_down, x, 0.0)
        return x

    def masked_half(half, x):
        return jnp.where(half_ok, x, 0.0) if half else x

    def gather(x, idx, axis):
        return jnp.take_along_axis(x, idx, axis=axis, mode="promise_in_bounds")

    def strip(side, half, pick):
        if half:
            x = jnp.where(lane < cols // 2, pick(bot_ref, side), pick(top_ref, side))
            return masked_half(1, x)
        return pick(mid_ref, side)

    TH[...] = jnp.zeros_like(TH)
    TH[0:theta_ref.shape[0], 0:members] = theta_ref[...]
    thp_ref[...] = TH[...].T[0:members]
    slot = sub * 8 + jnp.bitwise_and(lane, 7)
    par = [gather(jnp.broadcast_to(TH[k:k + 1, :], shape), slot, 1) for k in range(4)]
    diffuse = 0.05 * (1.0 + 0.5 * jnp.tanh(par[0]))
    hyper = 0.005 * (1.0 + 0.5 * jnp.tanh(par[1]))
    keep = 1.0 - 0.05 * (1.0 + 0.5 * jnp.tanh(par[2]))
    gain = par[3]
    mrow = jnp.concatenate([mode_ref[...], jnp.zeros((1, cols - members), jnp.int32)], axis=1)
    mrow = jnp.broadcast_to(mrow, shape)
    modes = [gather(mrow, sub * 8 + v, 1) for v in range(8)]

    block0 = lane - jnp.bitwise_and(lane, 7)
    for f in range(3):
        for j in range(n_rows // 8):
            if j == 0:
                x = jnp.where(has_up, ft_ref[pl.ds((8 + f) * DEPTH, 8), :], 0.0)
            elif j == n_rows // 8 - 1:
                x = jnp.where(has_down, fb_ref[pl.ds((8 + f) * DEPTH, 8), :], 0.0)
            else:
                x = f_ref[pl.ds((8 + f) * rows + (j - 1) * 8, 8), :]
            x = x if f == 2 else 0.5 * x
            for c in range(8):
                US[f, c, pl.ds(j * 8, 8), :] = gather(x, block0 + c, 1)
    scale = jnp.where(sub < 2, 0.5, 1.0)
    for side in range(2):
        for half in range(2):
            x = scale * strip(side, half, lambda ref, sd: ref[sd, members + 8:members + 16, :])
            for c in range(8):
                UH[side, c, half] = gather(x, block0 + c, 1)
            x = strip(side, half, lambda ref, sd: ref[sd, members:members + 8, :])
            ys = butterfly([gather(x, modes[v], 0) for v in range(8)])
            for c in range(8):
                FH[side, c, half] = gain * ys[c]
            ys = butterfly([strip(side, half, lambda ref, sd: ref[sd, pl.ds(v, 8, stride=8), :]) for v in range(8)])
            for c in range(8):
                H[0, side, c, half] = ys[c]

    for i in range(n_rows):
        if i < DEPTH:
            ref, per, k, fr = qt_ref, DEPTH, i, ft_ref
        elif i < DEPTH + rows:
            ref, per, k, fr = q_ref, rows, i - DEPTH, f_ref
        else:
            ref, per, k, fr = qb_ref, DEPTH, i - DEPTH - rows, fb_ref
        ys = butterfly([masked(i, ref[pl.ds(v * per + k, 8, stride=8 * per), :]) for v in range(8)])
        for c in range(8):
            Q[0, i, c] = ys[c]
        if 2 <= i < n_rows - 2:
            x = masked(i, fr[pl.ds(k, 8, stride=per), :])
            ys = butterfly([gather(x, modes[v], 0) for v in range(8)])
            for c in range(8):
                FO[i, c] = gain * ys[c]

    first, last = lane < 8, lane >= cols - 8

    def place(i):
        j = i - DEPTH
        return (0, j) if 0 <= j < rows else (1, (i - DEPTH - rows) % n_rows)

    def across(x, get, i):
        half, j = place(i)
        left = jnp.where(first, roll(get(0, 7, half), -8 * j), roll(x(7), 8))
        right = jnp.where(last, roll(get(1, 0, half), cols - 8 - 8 * j), roll(x(0), -8))
        return left, right

    def inward(x, lo, hi):
        left = [jnp.zeros(shape, F32)] * 2
        right = [jnp.zeros(shape, F32)] * 2
        for i in range(lo, hi):
            half, j = place(i)
            here = block0 == 8 * j
            left[half] = jnp.where(here, roll(x(i, 0), 8 * j), left[half])
            right[half] = jnp.where(here, roll(x(i, 7), 8 * j - (cols - 8)), right[half])
        return left, right

    def vertical(m, t):
        mn, tn, mp, tp = roll(m, -8), roll(t, -8), roll(m, 8), roll(t, 8)
        return ((jnp.where(last, tn, mn), jnp.where(last, mn, tn)),
                (jnp.where(first, tp, mp), jnp.where(first, mp, tp)))

    zero = jnp.zeros(shape, F32)

    def halo_x(get, ins, side, c, half):
        left, right = ins
        if c > 0:
            xm = get(side, c - 1, half)
        else:
            xm = right[half] if side == 1 else zero
        if c < 7:
            xp = get(side, c + 1, half)
        else:
            xp = left[half] if side == 0 else zero
        return xm, xp

    for s in range(STEPS):
        src, dst = s % 2, (s + 1) % 2
        lo, hi = 2 * s, n_rows - 2 * s
        final = s == STEPS - 1
        qa = lambda i, c: Q[src, i, c]
        qh = lambda side, c, half: H[src, side, c, half]
        lh = lambda side, c, half: LH[side, c, half]
        la = lambda i, c: L[i, c]
        ins = inward(qa, lo, hi)
        grads = {}
        for side in range(2):
            for c in range(8):
                m, t = qh(side, c, 0), qh(side, c, 1)
                nxt, prv = vertical(m, t)
                for half in range(2):
                    mid = (m, t)[half]
                    xm, xp = halo_x(qh, ins, side, c, half)
                    lap = (nxt[half] + prv[half]) + (xp + xm) - 4.0 * mid
                    LH[side, c, half] = masked_half(half, lap)
                    if not final:
                        grads[side, c, half] = (UH[side, c, half, 0:1] * (xp - xm)
                                                + UH[side, c, half, 1:2] * (nxt[half] - prv[half]))
        adv = {}
        def first_pass(i):
            left, right = across(lambda c: qa(i, c), qh, i)
            row = [qa(i, c) for c in range(8)]
            for c in range(8):
                xm = row[c - 1] if c else left
                xp = row[c + 1] if c < 7 else right
                up, dn = qa(i + 1, c), qa(i - 1, c)
                L[i, c] = masked(i, (up + dn) + (xp + xm) - 4.0 * row[c])
                if lo + 2 <= i < hi - 2:
                    adv[i, c] = (US[0, c, i:i + 1, :] * (xp - xm) + US[1, c, i:i + 1, :] * (up - dn))
                    adv[i, c] = keep * row[c] + (FO[i, c] - adv[i, c])

        def second_pass(i):
            left, right = across(lambda c: la(i, c), lh, i)
            row = [la(i, c) for c in range(8)]
            outs = []
            for c in range(8):
                xm = row[c - 1] if c else left
                xp = row[c + 1] if c < 7 else right
                bi = (la(i + 1, c) + la(i - 1, c)) + (xp + xm) - 4.0 * row[c]
                new = (adv.pop((i, c)) + (diffuse * row[c] - hyper * bi)) * US[2, c, i:i + 1, :]
                if final:
                    outs.append(new)
                else:
                    Q[dst, i, c] = new
            if final:
                for v, y in enumerate(butterfly(outs)):
                    out_ref[pl.ds(v * rows + i - DEPTH, 8, stride=8 * rows), :] = y

        first_pass(lo + 1)
        first_pass(lo + 2)
        for i in range(lo + 2, hi - 2):
            first_pass(i + 1)
            second_pass(i)
        if final:
            break
        ins = inward(la, lo + 1, hi - 1)
        for side in range(2):
            for c in range(8):
                m, t = lh(side, c, 0), lh(side, c, 1)
                nxt, prv = vertical(m, t)
                for half in range(2):
                    mid = (m, t)[half]
                    xm, xp = halo_x(lh, ins, side, c, half)
                    bi = (nxt[half] + prv[half]) + (xp + xm) - 4.0 * mid
                    new = (keep * qh(side, c, half) + (FH[side, c, half] - grads[side, c, half])
                           + (diffuse * mid - hyper * bi))
                    H[dst, side, c, half] = new * UH[side, c, half, 2:3]

    index = index_ref[0]
    col = jnp.bitwise_and(index, cols - 1)
    row = jnp.right_shift(index, cols.bit_length() - 1)
    hot = (lax.broadcasted_iota(jnp.int32, (cols, cols), 0) == col).astype(jnp.bfloat16)
    row_id = lax.broadcasted_iota(jnp.int32, (8, rows, cols), 1)
    dot = functools.partial(jnp.dot, preferred_element_type=F32)
    for g in range(members // 8):
        x = out_ref[pl.ds(g * 8 * rows, 8 * rows), :]
        x1 = x.astype(jnp.bfloat16)
        rem = x - x1.astype(F32)
        x2 = rem.astype(jnp.bfloat16)
        x3 = (rem - x2.astype(F32)).astype(jnp.bfloat16)
        picked = dot(x1, hot) + (dot(x2, hot) + dot(x3, hot))
        obs_ref[pl.ds(g * 8, 8), :] = jnp.sum(
            jnp.where(row_id == row[None], picked.reshape(8, rows, cols), 0.0), axis=1)


def run_model(mesh, state, fields, halos, member_mode, theta, obs_index):
    members, rows, cols = state.shape
    qt, qb, ft, fb, mid, top, bot = halos
    n_rows = rows + 2 * DEPTH
    sds = jax.ShapeDtypeStruct
    reg = (8, cols)
    out, obs, thp = pl.pallas_call(
        functools.partial(model_kernel, mesh.shape["gy"]),
        out_shape=[sds((members * rows, cols), F32), sds((members, cols), F32), sds((members, cols), F32)],
        in_specs=[vspec()] * 12,
        out_specs=[vspec()] * 3,
        scratch_shapes=[VM((2, n_rows, 8) + reg, F32), VM((n_rows, 8) + reg, F32), VM((n_rows, 8) + reg, F32),
                        VM((3, 8, n_rows, cols), F32),
                        VM((2, 2, 8, 2) + reg, F32), VM((2, 8, 2) + reg, F32), VM((2, 8, 2) + reg, F32),
                        VM((2, 8, 2) + reg, F32), VM((cols, cols), F32)],
        name="model",
    )(state.reshape(members * rows, cols), qt.reshape(-1, cols), qb.reshape(-1, cols),
      fields.reshape(-1, cols), ft.reshape(-1, cols), fb.reshape(-1, cols), mid, top, bot,
      member_mode.reshape(1, members), theta.T, obs_index)
    return out.reshape(members, rows, cols), obs, thp


def sums_kernel(n_gx, n_gy, n_ens, reduce_here, obs_ref, thp_ref, val_ref, sig_ref, full_ref, th_ref,
                obs_all, part, rs, ens_send, ens_recv, rs_send, rs_recv, ag_send, ag_recv):
    gx, gy, ens = lax.axis_index("gx"), lax.axis_index("gy"), lax.axis_index("ens")
    members = obs_ref.shape[0]
    n = n_gx * n_gy
    me = gy * n_gx + gx
    peers = [lax.rem(me + o, n) for o in range(1, n)] if reduce_here else []
    where = [{"gx": lax.rem(p, n_gx), "gy": lax.div(p, n_gx)} for p in peers]
    others = [lax.rem(ens + o, n_ens) for o in range(1, n_ens)]

    barrier = pltpu.get_barrier_semaphore()
    for p in others:
        pl.semaphore_signal(barrier, inc=1, device_id={"ens": p}, device_id_type=MESH)
    for p in where:
        pl.semaphore_signal(barrier, inc=1, device_id=p, device_id_type=MESH)
    pl.semaphore_wait(barrier, len(others) + len(where))

    def rdma(src, dst, send, recv, dev):
        return pltpu.make_async_remote_copy(src_ref=src, dst_ref=dst, send_sem=send, recv_sem=recv,
                                            device_id=dev, device_id_type=MESH)

    mine = pl.ds(pl.multiple_of(ens * members, members), members)
    copies = []
    for k, p in enumerate(others):
        copies.append(rdma(obs_ref, obs_all.at[mine], ens_send.at[2 * k], ens_recv.at[2 * k], {"ens": p}))
        copies.append(rdma(thp_ref, th_ref.at[mine], ens_send.at[2 * k + 1], ens_recv.at[2 * k + 1], {"ens": p}))
    for c in copies:
        c.start()
    obs_all[mine, :] = obs_ref[...]
    th_ref[mine, :] = thp_ref[...]
    for c in copies:
        c.wait()

    x = obs_all[...]
    mean = jnp.mean(x, axis=0, keepdims=True)
    inv = 1.0 / sig_ref[0]
    anom = (x - mean) * inv
    d = jnp.broadcast_to((val_ref[0] - mean) * inv, x.shape)
    nt = (((1,), (1,)), ((), ()))
    total = x.shape[0]
    part[:, 0:total] = lax.dot_general(anom, anom, nt, preferred_element_type=F32, precision=HIGH)
    part[:, total:] = lax.dot_general(anom, d, nt, preferred_element_type=F32, precision=HIGH)

    if not reduce_here:
        full_ref[...] = part[...]
        return
    own = total // n
    at = lambda p: pl.ds(pl.multiple_of(p * own, own), own)
    sends = [rdma(part.at[at(p)], rs.at[k], rs_send.at[k], rs_recv.at[k], w)
             for k, (p, w) in enumerate(zip(peers, where))]
    for c in sends:
        c.start()
    acc = part[at(me), :]
    for k, c in enumerate(sends):
        c.wait_recv()
        acc = acc + rs[k]
    full_ref[at(me), :] = acc
    gathers = [rdma(full_ref.at[at(me)], full_ref.at[at(me)], ag_send.at[k], ag_recv.at[k], w)
               for k, w in enumerate(where)]
    for c in gathers:
        c.start()
    for c in sends:
        c.wait_send()
    for c in gathers:
        c.wait()


def ensemble_sums(mesh, obs, thp, values, sigma):
    n_gx, n_gy, n_ens = mesh.shape["gx"], mesh.shape["gy"], mesh.shape["ens"]
    members, cols = obs.shape
    total = members * n_ens
    n = n_gx * n_gy
    reduce_here = total % (8 * n) == 0
    own = total // n if reduce_here else 8
    slots = n - 1 if reduce_here else 1
    full, th = pl.pallas_call(
        functools.partial(sums_kernel, n_gx, n_gy, n_ens, reduce_here),
        out_shape=[jax.ShapeDtypeStruct((total, 2 * total), F32), jax.ShapeDtypeStruct((total, cols), F32)],
        in_specs=[vspec()] * 4,
        out_specs=[vspec()] * 2,
        scratch_shapes=[VM((total, cols), F32), VM((total, 2 * total), F32), VM((slots, own, 2 * total), F32)]
        + [pltpu.SemaphoreType.DMA((2 * (n_ens - 1),))] * 2
        + [pltpu.SemaphoreType.DMA((slots,))] * 4,
        compiler_params=pltpu.CompilerParams(collective_id=1, has_side_effects=True),
        name="sums",
    )(obs, thp, values, sigma)
    if not reduce_here:
        full = lax.psum(full, ("gx", "gy"))
    return full, th


def solve_kernel(members, full_ref, th_ref, out_ref, xs):
    total = full_ref.shape[0]
    blocks = total // 8
    shape = (8, total)
    lane = lax.broadcasted_iota(jnp.int32, shape, 1)
    sub = lax.broadcasted_iota(jnp.int32, shape, 0)
    th = th_ref[...]
    mean = jnp.mean(th, axis=0, keepdims=True)
    A, R = [], []
    for k in range(blocks):
        rows = slice(8 * k, 8 * k + 8)
        A.append(full_ref[rows, 0:total] + jnp.where(lane == sub + 8 * k, float(total - 1), 0.0))
        R.append(th[rows] - mean)
    for k in range(blocks):
        pa, pr = A[k], R[k]
        for j in range(8):
            c = pa[:, 8 * k + j:8 * k + j + 1]
            inv = 1.0 / c[j:j + 1]
            na, nr = pa[j:j + 1] * inv, pr[j:j + 1] * inv
            pa = jnp.where(sub == j, na, pa - c * na)
            pr = jnp.where(sub == j, nr, pr - c * nr)
        A[k], R[k] = pa, pr
        for i in list(range(k + 1, blocks)) + list(range(k)):
            a, r = A[i], R[i]
            for j in range(8):
                c = A[i][:, 8 * k + j:8 * k + j + 1]
                a = a - c * pa[j:j + 1]
                r = r - c * pr[j:j + 1]
            A[i], R[i] = a, r
    shift = jnp.zeros((1, th.shape[1]), F32)
    for k in range(blocks):
        rows = slice(8 * k, 8 * k + 8)
        shift = shift + jnp.sum(full_ref[rows, total:] * R[k], axis=0, keepdims=True)
        xs[rows, :] = R[k]
    ens = lax.axis_index("ens")
    x = xs[pl.ds(pl.multiple_of(ens * members, members), members), :]
    new = mean + shift + float(total - 1) * x
    xs[0:members, :] = new
    out_ref[...] = xs[...].T[0:out_ref.shape[0], 0:members]


def solve(full, th, theta):
    return pl.pallas_call(
        functools.partial(solve_kernel, theta.shape[0]),
        out_shape=jax.ShapeDtypeStruct(theta.shape[::-1], F32),
        in_specs=[vspec()] * 2,
        out_specs=vspec(),
        scratch_shapes=[VM(th.shape, F32)],
        name="solve",
    )(full, th).T


def local(mesh, state, u_vel, v_vel, land, forcing, member_mode, theta, obs_index, obs_values, obs_sigma):
    ocean = (1 - land).astype(F32)
    rows, cols = u_vel.shape
    fields = jnp.concatenate([forcing, u_vel[None], v_vel[None], ocean[None], jnp.zeros((5, rows, cols), F32)], 0)
    halos = halo_exchange(mesh, state, fields)
    final, obs, thp = run_model(mesh, state, fields, halos, member_mode, theta, obs_index)
    full, th = ensemble_sums(mesh, obs, thp, obs_values, obs_sigma)
    return final, solve(full, th, theta)


def solution(mesh):
    placed = (
        P("ens", "gy", "gx"),
        P("gy", "gx"),
        P("gy", "gx"),
        P("gy", "gx"),
        P(None, "gy", "gx"),
        P("ens"),
        P("ens", None),
        P("gy", "gx", None),
        P("gy", "gx", None),
        P("gy", "gx", None),
    )
    return jax.shard_map(
        functools.partial(local, mesh),
        mesh=mesh,
        in_specs=placed,
        out_specs=(P("ens", "gy", "gx"), P("ens", None)),
        check_vma=False,
    )
```

```python
import functools
import jax
import jax.numpy as jnp
from jax import lax
from jax.experimental import pallas as pl
from jax.experimental.pallas import tpu as pltpu
from jax.sharding import PartitionSpec as P

STEPS = 4
DEPTH = 2 * STEPS
F32 = jnp.float32
VM = pltpu.VMEM
MESH = pl.DeviceIdType.MESH
HIGH = lax.Precision.HIGHEST


def vspec():
    return pl.BlockSpec(memory_space=pltpu.VMEM)


def halo_kernel(n_gx, n_gy, q_ref, forcing_ref, u_ref, v_ref, land_ref, f_ref, qt_ref, qb_ref, ft_ref, fb_ref, mid_ref, top_ref, bot_ref,
                pack, row_send, row_recv, gx_send, gx_recv, gy_send, gy_recv):
    gx, gy = lax.axis_index("gx"), lax.axis_index("gy")
    right, left = lax.rem(gx + 1, n_gx), lax.rem(gx + n_gx - 1, n_gx)
    has_up, has_down = gy > 0, gy < n_gy - 1
    up, down = jnp.maximum(gy - 1, 0), jnp.minimum(gy + 1, n_gy - 1)
    members, rows, cols = q_ref.shape
    fields = f_ref.shape[0]

    patterns = forcing_ref.shape[0]
    f_ref[0:patterns] = forcing_ref[...]
    f_ref[patterns] = u_ref[...]
    f_ref[patterns + 1] = v_ref[...]
    f_ref[patterns + 2] = (1 - land_ref[...]).astype(F32)
    f_ref[patterns + 3:] = jnp.zeros((fields - patterns - 3, rows, cols), F32)

    barrier = pltpu.get_barrier_semaphore()
    pl.semaphore_signal(barrier, inc=1, device_id={"gx": right}, device_id_type=MESH)
    pl.semaphore_signal(barrier, inc=1, device_id={"gx": left}, device_id_type=MESH)

    @pl.when(has_up)
    def _():
        pl.semaphore_signal(barrier, inc=1, device_id={"gy": up}, device_id_type=MESH)

    @pl.when(has_down)
    def _():
        pl.semaphore_signal(barrier, inc=1, device_id={"gy": down}, device_id_type=MESH)

    lane = lax.broadcasted_iota(jnp.int32, (8, cols), 1)

    def pack_from(ref, base):
        def body(g, carry):
            lo = jnp.zeros((8, cols), F32)
            hi = jnp.zeros((8, cols), F32)
            for r in range(rows):
                val = ref[pl.ds(g * 8, 8), r, :]
                mine = (lane // DEPTH) == r
                hi = jnp.where(mine, pltpu.roll(val, (r * DEPTH + DEPTH) % cols, 1), hi)
                lo = jnp.where(mine, pltpu.roll(val, (r * DEPTH) % cols, 1), lo)
            pack[0, pl.ds(base + g * 8, 8), :] = hi
            pack[1, pl.ds(base + g * 8, 8), :] = lo
            return carry
        lax.fori_loop(0, ref.shape[0] // 8, body, 0)

    pl.semaphore_wait(barrier, 2 + has_up.astype(jnp.int32) + has_down.astype(jnp.int32))

    def rdma(src, dst, send, recv, dev):
        return pltpu.make_async_remote_copy(src_ref=src, dst_ref=dst, send_sem=send, recv_sem=recv,
                                            device_id=dev, device_id_type=MESH)

    downs = [rdma(q_ref.at[:, rows - DEPTH:, :], qt_ref, row_send.at[0], row_recv.at[0], {"gy": down}),
             rdma(f_ref.at[:, rows - DEPTH:, :], ft_ref, row_send.at[1], row_recv.at[1], {"gy": down})]
    ups = [rdma(q_ref.at[:, :DEPTH, :], qb_ref, row_send.at[2], row_recv.at[2], {"gy": up}),
           rdma(f_ref.at[:, :DEPTH, :], fb_ref, row_send.at[3], row_recv.at[3], {"gy": up})]
    strip_down = rdma(mid_ref, top_ref, gy_send.at[0], gy_recv.at[0], {"gy": down})
    strip_up = rdma(mid_ref, bot_ref, gy_send.at[1], gy_recv.at[1], {"gy": up})

    @pl.when(has_down)
    def _():
        for c in downs:
            c.start()

    @pl.when(has_up)
    def _():
        for c in ups:
            c.start()

    pack_from(q_ref, 0)
    pack_from(f_ref, members)
    to_right = rdma(pack.at[0], mid_ref.at[0], gx_send.at[0], gx_recv.at[0], {"gx": right})
    to_left = rdma(pack.at[1], mid_ref.at[1], gx_send.at[1], gx_recv.at[1], {"gx": left})
    to_right.start()
    to_left.start()
    to_right.wait()
    to_left.wait()

    @pl.when(has_down)
    def _():
        strip_down.start()

    @pl.when(has_up)
    def _():
        strip_up.start()

    @pl.when(has_down)
    def _():
        for c in downs + [strip_down]:
            c.wait_send()
        for c in ups + [strip_up]:
            c.wait_recv()

    @pl.when(has_up)
    def _():
        for c in ups + [strip_up]:
            c.wait_send()
        for c in downs + [strip_down]:
            c.wait_recv()


def halo_exchange(mesh, state, forcing, u_vel, v_vel, land):
    members, rows, cols = state.shape
    nf = 16
    total = members + nf
    sds = jax.ShapeDtypeStruct
    return pl.pallas_call(
        functools.partial(halo_kernel, mesh.shape["gx"], mesh.shape["gy"]),
        out_shape=[sds((nf, rows, cols), F32), sds((members, DEPTH, cols), F32), sds((members, DEPTH, cols), F32),
                   sds((nf, DEPTH, cols), F32), sds((nf, DEPTH, cols), F32),
                   sds((2, total, cols), F32), sds((2, total, cols), F32), sds((2, total, cols), F32)],
        in_specs=[vspec()] * 5,
        out_specs=[vspec()] * 8,
        scratch_shapes=[VM((2, total, cols), F32)]
        + [pltpu.SemaphoreType.DMA((4,))] * 2
        + [pltpu.SemaphoreType.DMA((2,))] * 4,
        compiler_params=pltpu.CompilerParams(collective_id=0, has_side_effects=True),
        name="halo",
    )(state, forcing, u_vel, v_vel, land)


def model_kernel(n_gy, q_ref, qt_ref, qb_ref, f_ref, ft_ref, fb_ref, mid_ref, top_ref, bot_ref,
                 mode_ref, theta_ref, index_ref, out_ref, obs_ref,
                 Q, L, FO, US, H, LH, FH, UH, TH):
    gy = lax.axis_index("gy")
    members = mode_ref.shape[1]
    cols = q_ref.shape[1]
    rows = q_ref.shape[0] // members
    n_rows = rows + 2 * DEPTH
    has_up, has_down = gy > 0, gy < n_gy - 1
    shape = (8, cols)
    lane = lax.broadcasted_iota(jnp.int32, shape, 1)
    sub = lax.broadcasted_iota(jnp.int32, shape, 0)
    half_ok = jnp.where(lane < cols // 2, has_down.astype(jnp.int32), has_up.astype(jnp.int32)) > 0
    bits = {k: jnp.bitwise_and(lane, k) != 0 for k in (1, 2, 4)}

    def roll(x, k):
        return pltpu.roll(x, k % cols, 1)

    def butterfly(xs):
        xs = list(xs)
        for k in (1, 2, 4):
            for v in range(8):
                if not v & k:
                    x, y = xs[v], xs[v | k]
                    xs[v] = jnp.where(bits[k], roll(y, k), x)
                    xs[v | k] = jnp.where(bits[k], y, roll(x, -k))
        return xs

    def masked(i, x):
        if i < DEPTH:
            return jnp.where(has_up, x, 0.0)
        if i >= DEPTH + rows:
            return jnp.where(has_down, x, 0.0)
        return x

    def masked_half(half, x):
        return jnp.where(half_ok, x, 0.0) if half else x

    def gather(x, idx, axis):
        return jnp.take_along_axis(x, idx, axis=axis, mode="promise_in_bounds")

    def strip(side, half, pick):
        if half:
            x = jnp.where(lane < cols // 2, pick(bot_ref, side), pick(top_ref, side))
            return masked_half(1, x)
        return pick(mid_ref, side)

    TH[...] = jnp.zeros_like(TH)
    TH[0:theta_ref.shape[0], 0:members] = theta_ref[...]
    slot = sub * 8 + jnp.bitwise_and(lane, 7)
    par = [gather(jnp.broadcast_to(TH[k:k + 1, :], shape), slot, 1) for k in range(4)]
    diffuse = 0.05 * (1.0 + 0.5 * jnp.tanh(par[0]))
    hyper = 0.005 * (1.0 + 0.5 * jnp.tanh(par[1]))
    keep = 1.0 - 0.05 * (1.0 + 0.5 * jnp.tanh(par[2]))
    gain = par[3]
    mrow = jnp.concatenate([mode_ref[...], jnp.zeros((1, cols - members), jnp.int32)], axis=1)
    mrow = jnp.broadcast_to(mrow, shape)
    modes = [gather(mrow, sub * 8 + v, 1) for v in range(8)]

    block0 = lane - jnp.bitwise_and(lane, 7)
    for f in range(3):
        for j in range(n_rows // 8):
            if j == 0:
                x = jnp.where(has_up, ft_ref[pl.ds((8 + f) * DEPTH, 8), :], 0.0)
            elif j == n_rows // 8 - 1:
                x = jnp.where(has_down, fb_ref[pl.ds((8 + f) * DEPTH, 8), :], 0.0)
            else:
                x = f_ref[pl.ds((8 + f) * rows + (j - 1) * 8, 8), :]
            x = x if f == 2 else 0.5 * x
            for c in range(8):
                US[f, c, pl.ds(j * 8, 8), :] = gather(x, block0 + c, 1)
    scale = jnp.where(sub < 2, 0.5, 1.0)
    for side in range(2):
        for half in range(2):
            x = scale * strip(side, half, lambda ref, sd: ref[sd, members + 8:members + 16, :])
            for c in range(8):
                UH[side, c, half] = gather(x, block0 + c, 1)
            x = strip(side, half, lambda ref, sd: ref[sd, members:members + 8, :])
            ys = butterfly([gather(x, modes[v], 0) for v in range(8)])
            for c in range(8):
                FH[side, c, half] = gain * ys[c]
            ys = butterfly([strip(side, half, lambda ref, sd: ref[sd, pl.ds(v, 8, stride=8), :]) for v in range(8)])
            for c in range(8):
                H[0, side, c, half] = ys[c]

    for i in range(n_rows):
        if i < DEPTH:
            ref, per, k, fr = qt_ref, DEPTH, i, ft_ref
        elif i < DEPTH + rows:
            ref, per, k, fr = q_ref, rows, i - DEPTH, f_ref
        else:
            ref, per, k, fr = qb_ref, DEPTH, i - DEPTH - rows, fb_ref
        ys = butterfly([masked(i, ref[pl.ds(v * per + k, 8, stride=8 * per), :]) for v in range(8)])
        for c in range(8):
            Q[0, i, c] = ys[c]
        if 2 <= i < n_rows - 2:
            x = masked(i, fr[pl.ds(k, 8, stride=per), :])
            ys = butterfly([gather(x, modes[v], 0) for v in range(8)])
            for c in range(8):
                FO[i, c] = gain * ys[c]

    first, last = lane < 8, lane >= cols - 8

    def place(i):
        j = i - DEPTH
        return (0, j) if 0 <= j < rows else (1, (i - DEPTH - rows) % n_rows)

    def across(x, get, i):
        half, j = place(i)
        left = jnp.where(first, roll(get(0, 7, half), -8 * j), roll(x(7), 8))
        right = jnp.where(last, roll(get(1, 0, half), cols - 8 - 8 * j), roll(x(0), -8))
        return left, right

    def inward(x, lo, hi):
        left = [jnp.zeros(shape, F32)] * 2
        right = [jnp.zeros(shape, F32)] * 2
        for i in range(lo, hi):
            half, j = place(i)
            here = block0 == 8 * j
            left[half] = jnp.where(here, roll(x(i, 0), 8 * j), left[half])
            right[half] = jnp.where(here, roll(x(i, 7), 8 * j - (cols - 8)), right[half])
        return left, right

    def vertical(m, t):
        mn, tn, mp, tp = roll(m, -8), roll(t, -8), roll(m, 8), roll(t, 8)
        return ((jnp.where(last, tn, mn), jnp.where(last, mn, tn)),
                (jnp.where(first, tp, mp), jnp.where(first, mp, tp)))

    zero = jnp.zeros(shape, F32)

    def halo_x(get, ins, side, c, half):
        left, right = ins
        if c > 0:
            xm = get(side, c - 1, half)
        else:
            xm = right[half] if side == 1 else zero
        if c < 7:
            xp = get(side, c + 1, half)
        else:
            xp = left[half] if side == 0 else zero
        return xm, xp

    for s in range(STEPS):
        src, dst = s % 2, (s + 1) % 2
        lo, hi = 2 * s, n_rows - 2 * s
        final = s == STEPS - 1
        qa = lambda i, c: Q[src, i, c]
        qh = lambda side, c, half: H[src, side, c, half]
        lh = lambda side, c, half: LH[side, c, half]
        la = lambda i, c: L[i, c]
        ins = inward(qa, lo, hi)
        grads = {}
        for side in range(2):
            for c in range(8):
                m, t = qh(side, c, 0), qh(side, c, 1)
                nxt, prv = vertical(m, t)
                for half in range(2):
                    mid = (m, t)[half]
                    xm, xp = halo_x(qh, ins, side, c, half)
                    lap = (nxt[half] + prv[half]) + (xp + xm) - 4.0 * mid
                    LH[side, c, half] = masked_half(half, lap)
                    if not final:
                        grads[side, c, half] = (UH[side, c, half, 0:1] * (xp - xm)
                                                + UH[side, c, half, 1:2] * (nxt[half] - prv[half]))
        adv = {}
        def first_pass(i):
            left, right = across(lambda c: qa(i, c), qh, i)
            row = [qa(i, c) for c in range(8)]
            for c in range(8):
                xm = row[c - 1] if c else left
                xp = row[c + 1] if c < 7 else right
                up, dn = qa(i + 1, c), qa(i - 1, c)
                L[i, c] = masked(i, (up + dn) + (xp + xm) - 4.0 * row[c])
                if lo + 2 <= i < hi - 2:
                    adv[i, c] = (US[0, c, i:i + 1, :] * (xp - xm) + US[1, c, i:i + 1, :] * (up - dn))
                    adv[i, c] = keep * row[c] + (FO[i, c] - adv[i, c])

        def second_pass(i):
            left, right = across(lambda c: la(i, c), lh, i)
            row = [la(i, c) for c in range(8)]
            outs = []
            for c in range(8):
                xm = row[c - 1] if c else left
                xp = row[c + 1] if c < 7 else right
                bi = (la(i + 1, c) + la(i - 1, c)) + (xp + xm) - 4.0 * row[c]
                new = (adv.pop((i, c)) + (diffuse * row[c] - hyper * bi)) * US[2, c, i:i + 1, :]
                if final:
                    outs.append(new)
                else:
                    Q[dst, i, c] = new
            if final:
                for v, y in enumerate(butterfly(outs)):
                    out_ref[pl.ds(v * rows + i - DEPTH, 8, stride=8 * rows), :] = y

        first_pass(lo + 1)
        first_pass(lo + 2)
        for i in range(lo + 2, hi - 2):
            first_pass(i + 1)
            second_pass(i)
        if final:
            break
        ins = inward(la, lo + 1, hi - 1)
        for side in range(2):
            for c in range(8):
                m, t = lh(side, c, 0), lh(side, c, 1)
                nxt, prv = vertical(m, t)
                for half in range(2):
                    mid = (m, t)[half]
                    xm, xp = halo_x(lh, ins, side, c, half)
                    bi = (nxt[half] + prv[half]) + (xp + xm) - 4.0 * mid
                    new = (keep * qh(side, c, half) + (FH[side, c, half] - grads[side, c, half])
                           + (diffuse * mid - hyper * bi))
                    H[dst, side, c, half] = new * UH[side, c, half, 2:3]

    index = index_ref[0]
    col = jnp.bitwise_and(index, cols - 1)
    row = jnp.right_shift(index, cols.bit_length() - 1)
    hot = (lax.broadcasted_iota(jnp.int32, (cols, cols), 0) == col).astype(jnp.bfloat16)
    row_id = lax.broadcasted_iota(jnp.int32, (8, rows, cols), 1)
    dot = functools.partial(jnp.dot, preferred_element_type=F32)
    for g in range(members // 8):
        x = out_ref[pl.ds(g * 8 * rows, 8 * rows), :]
        x1 = x.astype(jnp.bfloat16)
        rem = x - x1.astype(F32)
        x2 = rem.astype(jnp.bfloat16)
        x3 = (rem - x2.astype(F32)).astype(jnp.bfloat16)
        picked = dot(x1, hot) + (dot(x2, hot) + dot(x3, hot))
        obs_ref[pl.ds(g * 8, 8), :] = jnp.sum(
            jnp.where(row_id == row[None], picked.reshape(8, rows, cols), 0.0), axis=1)


def run_model(mesh, state, fields, halos, member_mode, theta, obs_index):
    members, rows, cols = state.shape
    qt, qb, ft, fb, mid, top, bot = halos
    n_rows = rows + 2 * DEPTH
    sds = jax.ShapeDtypeStruct
    reg = (8, cols)
    out, obs = pl.pallas_call(
        functools.partial(model_kernel, mesh.shape["gy"]),
        out_shape=[sds((members * rows, cols), F32), sds((members, cols), F32)],
        in_specs=[vspec()] * 12,
        out_specs=[vspec()] * 2,
        scratch_shapes=[VM((2, n_rows, 8) + reg, F32), VM((n_rows, 8) + reg, F32), VM((n_rows, 8) + reg, F32),
                        VM((3, 8, n_rows, cols), F32),
                        VM((2, 2, 8, 2) + reg, F32), VM((2, 8, 2) + reg, F32), VM((2, 8, 2) + reg, F32),
                        VM((2, 8, 2) + reg, F32), VM(reg, F32)],
        name="model",
    )(state.reshape(members * rows, cols), qt.reshape(-1, cols), qb.reshape(-1, cols),
      fields.reshape(-1, cols), ft.reshape(-1, cols), fb.reshape(-1, cols), mid, top, bot,
      member_mode.reshape(1, members), theta.T, obs_index)
    return out.reshape(members, rows, cols), obs


def sums_kernel(n_gx, n_gy, n_ens, reduce_here, obs_ref, theta_ref, val_ref, sig_ref, full_ref, c_ref, th_ref,
                obs_all, part, rs, c_own, cs, ens_send, ens_recv, rs_send, rs_recv, cs_send, cs_recv, ag_send, ag_recv):
    gx, gy, ens = lax.axis_index("gx"), lax.axis_index("gy"), lax.axis_index("ens")
    members = obs_ref.shape[0]
    n = n_gx * n_gy
    me = gy * n_gx + gx
    peers = [lax.rem(me + o, n) for o in range(1, n)] if reduce_here else []
    where = [{"gx": lax.rem(p, n_gx), "gy": lax.div(p, n_gx)} for p in peers]
    others = [lax.rem(ens + o, n_ens) for o in range(1, n_ens)]

    barrier = pltpu.get_barrier_semaphore()
    for p in others:
        pl.semaphore_signal(barrier, inc=1, device_id={"ens": p}, device_id_type=MESH)
    for p in where:
        pl.semaphore_signal(barrier, inc=1, device_id=p, device_id_type=MESH)
    pl.semaphore_wait(barrier, len(others) + len(where))

    def rdma(src, dst, send, recv, dev):
        return pltpu.make_async_remote_copy(src_ref=src, dst_ref=dst, send_sem=send, recv_sem=recv,
                                            device_id=dev, device_id_type=MESH)

    mine = pl.ds(pl.multiple_of(ens * members, members), members)
    obs_copies, th_copies = [], []
    for k, p in enumerate(others):
        obs_copies.append(rdma(obs_ref, obs_all.at[mine], ens_send.at[2 * k], ens_recv.at[2 * k], {"ens": p}))
        th_copies.append(rdma(theta_ref, th_ref.at[ens], ens_send.at[2 * k + 1], ens_recv.at[2 * k + 1], {"ens": p}))
    for c in obs_copies + th_copies:
        c.start()
    obs_all[mine, :] = obs_ref[...]
    th_ref[ens] = theta_ref[...]
    for c in obs_copies:
        c.wait()

    x = obs_all[...]
    mean = jnp.mean(x, axis=0, keepdims=True)
    inv = 1.0 / sig_ref[0]
    anom = (x - mean) * inv
    d = jnp.broadcast_to((val_ref[0] - mean) * inv, (8, x.shape[1]))
    nt = (((1,), (1,)), ((), ()))
    total = x.shape[0]
    c_part = lax.dot_general(d, anom, nt, preferred_element_type=F32, precision=HIGH)[0:1]
    gram = lax.dot_general(anom, anom, nt, preferred_element_type=F32, precision=HIGH)

    if not reduce_here:
        full_ref[...] = gram
        c_ref[...] = c_part
        for c in th_copies:
            c.wait()
        return
    c_own[...] = c_part
    part[...] = gram
    own = total // n
    at = lambda p: pl.ds(pl.multiple_of(p * own, own), own)
    sends = [rdma(part.at[at(p)], rs.at[k], rs_send.at[k], rs_recv.at[k], w)
             for k, (p, w) in enumerate(zip(peers, where))]
    c_sends = [rdma(c_own, cs.at[k], cs_send.at[k], cs_recv.at[k], w) for k, w in enumerate(where)]
    for c in sends + c_sends:
        c.start()
    acc = part[at(me), :]
    for k, c in enumerate(sends):
        c.wait_recv()
        acc = acc + rs[k]
    full_ref[at(me), :] = acc
    gathers = [rdma(full_ref.at[at(me)], full_ref.at[at(me)], ag_send.at[k], ag_recv.at[k], w)
               for k, w in enumerate(where)]
    for c in gathers:
        c.start()
    acc = c_own[...]
    for k, c in enumerate(c_sends):
        c.wait_recv()
        acc = acc + cs[k]
    c_ref[...] = acc
    for c in sends + c_sends:
        c.wait_send()
    for c in th_copies + gathers:
        c.wait()


def ensemble_sums(mesh, obs, theta, values, sigma):
    n_gx, n_gy, n_ens = mesh.shape["gx"], mesh.shape["gy"], mesh.shape["ens"]
    members, cols = obs.shape
    total = members * n_ens
    n = n_gx * n_gy
    reduce_here = total % (8 * n) == 0
    own = total // n if reduce_here else 8
    slots = n - 1 if reduce_here else 1
    sds = jax.ShapeDtypeStruct
    full, c, th = pl.pallas_call(
        functools.partial(sums_kernel, n_gx, n_gy, n_ens, reduce_here),
        out_shape=[sds((total, total), F32), sds((1, total), F32), sds((n_ens,) + theta.shape[::-1], F32)],
        in_specs=[vspec()] * 4,
        out_specs=[vspec()] * 3,
        scratch_shapes=[VM((total, cols), F32), VM((total, total), F32), VM((slots, own, total), F32),
                        VM((1, total), F32), VM((slots, 1, total), F32)]
        + [pltpu.SemaphoreType.DMA((2 * (n_ens - 1),))] * 2
        + [pltpu.SemaphoreType.DMA((slots,))] * 6,
        compiler_params=pltpu.CompilerParams(collective_id=1, has_side_effects=True),
        name="sums",
    )(obs, theta.T, values, sigma)
    if not reduce_here:
        full, c = lax.psum((full, c), ("gx", "gy"))
    return full, c, th


def solve_kernel(members, full_ref, c_ref, th_ref, out_ref, xs):
    total = full_ref.shape[0]
    blocks = total // 8
    n_ens, params = th_ref.shape[0], th_ref.shape[1]
    shape = (8, total)
    lane = lax.broadcasted_iota(jnp.int32, shape, 1)
    sub = lax.broadcasted_iota(jnp.int32, shape, 0)
    tht = jnp.concatenate([th_ref[e] for e in range(n_ens)], axis=1)
    spread = tht - jnp.mean(tht, axis=1, keepdims=True)
    xs[...] = jnp.zeros_like(xs)
    xs[0:params, :] = spread
    cols_of = xs[...].T
    A, R = [], []
    for k in range(blocks):
        rows = slice(8 * k, 8 * k + 8)
        A.append(full_ref[rows, :] + jnp.where(lane == sub + 8 * k, float(total - 1), 0.0))
        R.append(cols_of[rows])

    def splat(x):
        return jnp.broadcast_to(x, shape)

    for k in range(blocks):
        rs_, rr = [], []
        d = {}
        for j in range(8):
            row = splat(A[k][j:j + 1])
            rs_.append(row)
            rr.append(splat(R[k][j:j + 1]))
            for i in range(j, 8):
                d[j, i] = splat(row[:, 8 * k + i:8 * k + i + 1])
        inv = []
        for j in range(8):
            inv.append(1.0 / d[j, j])
            for i in range(j + 1, 8):
                m = d[j, i] * inv[j]
                rs_[i] = rs_[i] - m * rs_[j]
                rr[i] = rr[i] - m * rr[j]
                for q in range(i, 8):
                    d[i, q] = d[i, q] - m * d[j, q]
        for i in reversed(range(8)):
            for j in range(i + 1, 8):
                rs_[i] = rs_[i] - d[i, j] * rs_[j]
                rr[i] = rr[i] - d[i, j] * rr[j]
            rs_[i] = rs_[i] * inv[i]
            rr[i] = rr[i] * inv[i]
        a, r = rs_[7], rr[7]
        for j in range(7):
            a = jnp.where(sub == j, rs_[j], a)
            r = jnp.where(sub == j, rr[j], r)
        A[k], R[k] = a, r
        for i in list(range(k + 1, blocks)) + list(range(k)):
            a, r = A[i], R[i]
            for j in range(8):
                c = splat(A[i][:, 8 * k + j:8 * k + j + 1])
                if k + 1 < blocks:
                    a = a - c * rs_[j]
                r = r - c * rr[j]
            A[i], R[i] = a, r
    for k in range(blocks):
        xs[8 * k:8 * k + 8, :] = R[k]
    x = xs[...].T[0:8]
    shift = jnp.sum(x * c_ref[...], axis=1, keepdims=True)
    new = (jnp.mean(tht, axis=1, keepdims=True) + shift[0:params]) + float(total - 1) * x[0:params]
    ens = lax.axis_index("ens")
    for e in range(n_ens):
        @pl.when(ens == e)
        def _():
            out_ref[...] = new[:, e * members:(e + 1) * members]


def solve(full, c, th, theta):
    return pl.pallas_call(
        functools.partial(solve_kernel, theta.shape[0]),
        out_shape=jax.ShapeDtypeStruct(theta.shape[::-1], F32),
        in_specs=[vspec()] * 3,
        out_specs=vspec(),
        scratch_shapes=[VM(full.shape, F32)],
        name="solve",
    )(full, c, th).T


def local(mesh, state, u_vel, v_vel, land, forcing, member_mode, theta, obs_index, obs_values, obs_sigma):
    fields, *halos = halo_exchange(mesh, state, forcing, u_vel, v_vel, land)
    final, obs = run_model(mesh, state, fields, halos, member_mode, theta, obs_index)
    full, c, th = ensemble_sums(mesh, obs, theta, obs_values, obs_sigma)
    return final, solve(full, c, th, theta)


def solution(mesh):
    placed = (
        P("ens", "gy", "gx"),
        P("gy", "gx"),
        P("gy", "gx"),
        P("gy", "gx"),
        P(None, "gy", "gx"),
        P("ens"),
        P("ens", None),
        P("gy", "gx", None),
        P("gy", "gx", None),
        P("gy", "gx", None),
    )
    return jax.shard_map(
        functools.partial(local, mesh),
        mesh=mesh,
        in_specs=placed,
        out_specs=(P("ens", "gy", "gx"), P("ens", None)),
        check_vma=False,
    )
```

```python
import functools
import jax
import jax.numpy as jnp
from jax import lax
from jax.experimental import pallas as pl
from jax.experimental.pallas import tpu as pltpu
from jax.sharding import PartitionSpec as P

STEPS = 4
DEPTH = 2 * STEPS
F32 = jnp.float32
VM = pltpu.VMEM
MESH = pl.DeviceIdType.MESH
HIGH = lax.Precision.HIGHEST


def vspec():
    return pl.BlockSpec(memory_space=pltpu.VMEM)


def halo_kernel(n_gx, n_gy, q_ref, forcing_ref, u_ref, v_ref, land_ref, f_ref, qt_ref, qb_ref, ft_ref, fb_ref, mid_ref, top_ref, bot_ref,
                pack, row_send, row_recv, gx_send, gx_recv, gy_send, gy_recv):
    gx, gy = lax.axis_index("gx"), lax.axis_index("gy")
    right, left = lax.rem(gx + 1, n_gx), lax.rem(gx + n_gx - 1, n_gx)
    has_up, has_down = gy > 0, gy < n_gy - 1
    up, down = jnp.maximum(gy - 1, 0), jnp.minimum(gy + 1, n_gy - 1)
    members, rows, cols = q_ref.shape
    fields = f_ref.shape[0]

    patterns = forcing_ref.shape[0]
    f_ref[0:patterns] = forcing_ref[...]
    f_ref[patterns] = u_ref[...]
    f_ref[patterns + 1] = v_ref[...]
    f_ref[patterns + 2] = (1 - land_ref[...]).astype(F32)
    f_ref[patterns + 3:] = jnp.zeros((fields - patterns - 3, rows, cols), F32)

    barrier = pltpu.get_barrier_semaphore()
    pl.semaphore_signal(barrier, inc=1, device_id={"gx": right}, device_id_type=MESH)
    pl.semaphore_signal(barrier, inc=1, device_id={"gx": left}, device_id_type=MESH)

    @pl.when(has_up)
    def _():
        pl.semaphore_signal(barrier, inc=1, device_id={"gy": up}, device_id_type=MESH)

    @pl.when(has_down)
    def _():
        pl.semaphore_signal(barrier, inc=1, device_id={"gy": down}, device_id_type=MESH)

    lane = lax.broadcasted_iota(jnp.int32, (8, cols), 1)

    def pack_from(ref, base):
        def body(g, carry):
            lo = jnp.zeros((8, cols), F32)
            hi = jnp.zeros((8, cols), F32)
            for r in range(rows):
                val = ref[pl.ds(g * 8, 8), r, :]
                mine = (lane // DEPTH) == r
                hi = jnp.where(mine, pltpu.roll(val, (r * DEPTH + DEPTH) % cols, 1), hi)
                lo = jnp.where(mine, pltpu.roll(val, (r * DEPTH) % cols, 1), lo)
            pack[0, pl.ds(base + g * 8, 8), :] = hi
            pack[1, pl.ds(base + g * 8, 8), :] = lo
            return carry
        lax.fori_loop(0, ref.shape[0] // 8, body, 0)

    pl.semaphore_wait(barrier, 2 + has_up.astype(jnp.int32) + has_down.astype(jnp.int32))

    def rdma(src, dst, send, recv, dev):
        return pltpu.make_async_remote_copy(src_ref=src, dst_ref=dst, send_sem=send, recv_sem=recv,
                                            device_id=dev, device_id_type=MESH)

    downs = [rdma(q_ref.at[:, rows - DEPTH:, :], qt_ref, row_send.at[0], row_recv.at[0], {"gy": down}),
             rdma(f_ref.at[:, rows - DEPTH:, :], ft_ref, row_send.at[1], row_recv.at[1], {"gy": down})]
    ups = [rdma(q_ref.at[:, :DEPTH, :], qb_ref, row_send.at[2], row_recv.at[2], {"gy": up}),
           rdma(f_ref.at[:, :DEPTH, :], fb_ref, row_send.at[3], row_recv.at[3], {"gy": up})]
    strip_down = rdma(mid_ref, top_ref, gy_send.at[0], gy_recv.at[0], {"gy": down})
    strip_up = rdma(mid_ref, bot_ref, gy_send.at[1], gy_recv.at[1], {"gy": up})

    @pl.when(has_down)
    def _():
        for c in downs:
            c.start()

    @pl.when(has_up)
    def _():
        for c in ups:
            c.start()

    pack_from(q_ref, 0)
    pack_from(f_ref, members)
    to_right = rdma(pack.at[0], mid_ref.at[0], gx_send.at[0], gx_recv.at[0], {"gx": right})
    to_left = rdma(pack.at[1], mid_ref.at[1], gx_send.at[1], gx_recv.at[1], {"gx": left})
    to_right.start()
    to_left.start()
    to_right.wait()
    to_left.wait()

    @pl.when(has_down)
    def _():
        strip_down.start()

    @pl.when(has_up)
    def _():
        strip_up.start()

    @pl.when(has_down)
    def _():
        for c in downs + [strip_down]:
            c.wait_send()
        for c in ups + [strip_up]:
            c.wait_recv()

    @pl.when(has_up)
    def _():
        for c in ups + [strip_up]:
            c.wait_send()
        for c in downs + [strip_down]:
            c.wait_recv()


def halo_exchange(mesh, state, forcing, u_vel, v_vel, land):
    members, rows, cols = state.shape
    nf = 16
    total = members + nf
    sds = jax.ShapeDtypeStruct
    return pl.pallas_call(
        functools.partial(halo_kernel, mesh.shape["gx"], mesh.shape["gy"]),
        out_shape=[sds((nf, rows, cols), F32), sds((members, DEPTH, cols), F32), sds((members, DEPTH, cols), F32),
                   sds((nf, DEPTH, cols), F32), sds((nf, DEPTH, cols), F32),
                   sds((2, total, cols), F32), sds((2, total, cols), F32), sds((2, total, cols), F32)],
        in_specs=[vspec()] * 5,
        out_specs=[vspec()] * 8,
        scratch_shapes=[VM((2, total, cols), F32)]
        + [pltpu.SemaphoreType.DMA((4,))] * 2
        + [pltpu.SemaphoreType.DMA((2,))] * 4,
        compiler_params=pltpu.CompilerParams(collective_id=0, has_side_effects=True),
        name="halo",
    )(state, forcing, u_vel, v_vel, land)


def model_kernel(n_gy, q_ref, qt_ref, qb_ref, f_ref, ft_ref, fb_ref, mid_ref, top_ref, bot_ref,
                 mode_ref, theta_ref, index_ref, out_ref, obs_ref,
                 Q, L, FO, US, H, LH, FH, UH, TH):
    gy = lax.axis_index("gy")
    members = mode_ref.shape[1]
    cols = q_ref.shape[1]
    rows = q_ref.shape[0] // members
    n_rows = rows + 2 * DEPTH
    has_up, has_down = gy > 0, gy < n_gy - 1
    shape = (8, cols)
    lane = lax.broadcasted_iota(jnp.int32, shape, 1)
    sub = lax.broadcasted_iota(jnp.int32, shape, 0)
    half_ok = jnp.where(lane < cols // 2, has_down.astype(jnp.int32), has_up.astype(jnp.int32)) > 0
    bits = {k: jnp.bitwise_and(lane, k) != 0 for k in (1, 2, 4)}

    def roll(x, k):
        return pltpu.roll(x, k % cols, 1)

    def butterfly(xs):
        xs = list(xs)
        for k in (1, 2, 4):
            for v in range(8):
                if not v & k:
                    x, y = xs[v], xs[v | k]
                    xs[v] = jnp.where(bits[k], roll(y, k), x)
                    xs[v | k] = jnp.where(bits[k], y, roll(x, -k))
        return xs

    def masked(i, x):
        if i < DEPTH:
            return jnp.where(has_up, x, 0.0)
        if i >= DEPTH + rows:
            return jnp.where(has_down, x, 0.0)
        return x

    def masked_half(half, x):
        return jnp.where(half_ok, x, 0.0) if half else x

    def gather(x, idx, axis):
        return jnp.take_along_axis(x, idx, axis=axis, mode="promise_in_bounds")

    def strip(side, half, pick):
        if half:
            x = jnp.where(lane < cols // 2, pick(bot_ref, side), pick(top_ref, side))
            return masked_half(1, x)
        return pick(mid_ref, side)

    TH[...] = jnp.zeros_like(TH)
    TH[0:theta_ref.shape[0], 0:members] = theta_ref[...]
    slot = sub * 8 + jnp.bitwise_and(lane, 7)
    par = [gather(jnp.broadcast_to(TH[k:k + 1, :], shape), slot, 1) for k in range(4)]
    diffuse = 0.05 * (1.0 + 0.5 * jnp.tanh(par[0]))
    hyper = 0.005 * (1.0 + 0.5 * jnp.tanh(par[1]))
    keep = 1.0 - 0.05 * (1.0 + 0.5 * jnp.tanh(par[2]))
    gain = par[3]
    mrow = jnp.concatenate([mode_ref[...], jnp.zeros((1, cols - members), jnp.int32)], axis=1)
    mrow = jnp.broadcast_to(mrow, shape)
    modes = [gather(mrow, sub * 8 + v, 1) for v in range(8)]

    block0 = lane - jnp.bitwise_and(lane, 7)
    for f in range(3):
        for j in range(n_rows // 8):
            if j == 0:
                x = jnp.where(has_up, ft_ref[pl.ds((8 + f) * DEPTH, 8), :], 0.0)
            elif j == n_rows // 8 - 1:
                x = jnp.where(has_down, fb_ref[pl.ds((8 + f) * DEPTH, 8), :], 0.0)
            else:
                x = f_ref[pl.ds((8 + f) * rows + (j - 1) * 8, 8), :]
            x = x if f == 2 else 0.5 * x
            for c in range(8):
                US[f, c, pl.ds(j * 8, 8), :] = gather(x, block0 + c, 1)
    scale = jnp.where(sub < 2, 0.5, 1.0)
    for side in range(2):
        for half in range(2):
            x = scale * strip(side, half, lambda ref, sd: ref[sd, members + 8:members + 16, :])
            for c in range(8):
                UH[side, c, half] = gather(x, block0 + c, 1)
            x = strip(side, half, lambda ref, sd: ref[sd, members:members + 8, :])
            ys = butterfly([gather(x, modes[v], 0) for v in range(8)])
            for c in range(8):
                FH[side, c, half] = gain * ys[c]
            ys = butterfly([strip(side, half, lambda ref, sd: ref[sd, pl.ds(v, 8, stride=8), :]) for v in range(8)])
            for c in range(8):
                H[0, side, c, half] = ys[c]

    def enter(ref, per, fr, base, ok):
        def body(k, carry):
            def keep_in(x):
                return x if ok is None else jnp.where(ok, x, 0.0)
            ys = butterfly([keep_in(ref[pl.ds(v * per + k, 8, stride=8 * per), :]) for v in range(8)])
            x = keep_in(fr[pl.ds(k, 8, stride=per), :])
            zs = butterfly([gather(x, modes[v], 0) for v in range(8)])
            for c in range(8):
                Q[0, base + k, c] = ys[c]
                FO[base + k, c] = gain * zs[c]
            return carry
        lax.fori_loop(0, per, body, 0)

    enter(qt_ref, DEPTH, ft_ref, 0, has_up)
    enter(q_ref, rows, f_ref, DEPTH, None)
    enter(qb_ref, DEPTH, fb_ref, DEPTH + rows, has_down)

    first, last = lane < 8, lane >= cols - 8

    def place(i):
        j = i - DEPTH
        return (0, j) if 0 <= j < rows else (1, (i - DEPTH - rows) % n_rows)

    def across(x, get, i):
        half, j = place(i)
        left = jnp.where(first, roll(get(0, 7, half), -8 * j), roll(x(7), 8))
        right = jnp.where(last, roll(get(1, 0, half), cols - 8 - 8 * j), roll(x(0), -8))
        return left, right

    def inward(x, lo, hi):
        left = [jnp.zeros(shape, F32)] * 2
        right = [jnp.zeros(shape, F32)] * 2
        for i in range(lo, hi):
            half, j = place(i)
            here = block0 == 8 * j
            left[half] = jnp.where(here, roll(x(i, 0), 8 * j), left[half])
            right[half] = jnp.where(here, roll(x(i, 7), 8 * j - (cols - 8)), right[half])
        return left, right

    def vertical(m, t):
        mn, tn, mp, tp = roll(m, -8), roll(t, -8), roll(m, 8), roll(t, 8)
        return ((jnp.where(last, tn, mn), jnp.where(last, mn, tn)),
                (jnp.where(first, tp, mp), jnp.where(first, mp, tp)))

    zero = jnp.zeros(shape, F32)

    def halo_x(get, ins, side, c, half):
        left, right = ins
        if c > 0:
            xm = get(side, c - 1, half)
        else:
            xm = right[half] if side == 1 else zero
        if c < 7:
            xp = get(side, c + 1, half)
        else:
            xp = left[half] if side == 0 else zero
        return xm, xp

    for s in range(STEPS):
        src, dst = s % 2, (s + 1) % 2
        lo, hi = 2 * s, n_rows - 2 * s
        final = s == STEPS - 1
        qa = lambda i, c: Q[src, i, c]
        qh = lambda side, c, half: H[src, side, c, half]
        lh = lambda side, c, half: LH[side, c, half]
        la = lambda i, c: L[i, c]
        ins = inward(qa, lo, hi)
        grads = {}
        for side in range(2):
            for c in range(8):
                m, t = qh(side, c, 0), qh(side, c, 1)
                nxt, prv = vertical(m, t)
                for half in range(2):
                    mid = (m, t)[half]
                    xm, xp = halo_x(qh, ins, side, c, half)
                    lap = (nxt[half] + prv[half]) + (xp + xm) - 4.0 * mid
                    LH[side, c, half] = masked_half(half, lap)
                    if not final:
                        grads[side, c, half] = (UH[side, c, half, 0:1] * (xp - xm)
                                                + UH[side, c, half, 1:2] * (nxt[half] - prv[half]))
        adv = {}
        def first_pass(i):
            left, right = across(lambda c: qa(i, c), qh, i)
            row = [qa(i, c) for c in range(8)]
            for c in range(8):
                xm = row[c - 1] if c else left
                xp = row[c + 1] if c < 7 else right
                up, dn = qa(i + 1, c), qa(i - 1, c)
                L[i, c] = masked(i, (up + dn) + (xp + xm) - 4.0 * row[c])
                if lo + 2 <= i < hi - 2:
                    adv[i, c] = (US[0, c, i:i + 1, :] * (xp - xm) + US[1, c, i:i + 1, :] * (up - dn))
                    adv[i, c] = keep * row[c] + (FO[i, c] - adv[i, c])

        def second_pass(i):
            left, right = across(lambda c: la(i, c), lh, i)
            row = [la(i, c) for c in range(8)]
            outs = []
            for c in range(8):
                xm = row[c - 1] if c else left
                xp = row[c + 1] if c < 7 else right
                bi = (la(i + 1, c) + la(i - 1, c)) + (xp + xm) - 4.0 * row[c]
                new = (adv.pop((i, c)) + (diffuse * row[c] - hyper * bi)) * US[2, c, i:i + 1, :]
                if final:
                    outs.append(new)
                else:
                    Q[dst, i, c] = new
            if final:
                for v, y in enumerate(butterfly(outs)):
                    out_ref[pl.ds(v * rows + i - DEPTH, 8, stride=8 * rows), :] = y

        first_pass(lo + 1)
        first_pass(lo + 2)
        for i in range(lo + 2, hi - 2):
            first_pass(i + 1)
            second_pass(i)
        if final:
            break
        ins = inward(la, lo + 1, hi - 1)
        for side in range(2):
            for c in range(8):
                m, t = lh(side, c, 0), lh(side, c, 1)
                nxt, prv = vertical(m, t)
                for half in range(2):
                    mid = (m, t)[half]
                    xm, xp = halo_x(lh, ins, side, c, half)
                    bi = (nxt[half] + prv[half]) + (xp + xm) - 4.0 * mid
                    new = (keep * qh(side, c, half) + (FH[side, c, half] - grads[side, c, half])
                           + (diffuse * mid - hyper * bi))
                    H[dst, side, c, half] = new * UH[side, c, half, 2:3]

    index = index_ref[0]
    col = jnp.bitwise_and(index, cols - 1)
    row = jnp.right_shift(index, cols.bit_length() - 1)
    hot = (lax.broadcasted_iota(jnp.int32, (cols, cols), 0) == col).astype(jnp.bfloat16)
    row_id = lax.broadcasted_iota(jnp.int32, (8, rows, cols), 1)
    dot = functools.partial(jnp.dot, preferred_element_type=F32)
    for g in range(members // 8):
        x = out_ref[pl.ds(g * 8 * rows, 8 * rows), :]
        x1 = x.astype(jnp.bfloat16)
        rem = x - x1.astype(F32)
        x2 = rem.astype(jnp.bfloat16)
        x3 = (rem - x2.astype(F32)).astype(jnp.bfloat16)
        picked = dot(x1, hot) + (dot(x2, hot) + dot(x3, hot))
        obs_ref[pl.ds(g * 8, 8), :] = jnp.sum(
            jnp.where(row_id == row[None], picked.reshape(8, rows, cols), 0.0), axis=1)


def run_model(mesh, state, fields, halos, member_mode, theta, obs_index):
    members, rows, cols = state.shape
    qt, qb, ft, fb, mid, top, bot = halos
    n_rows = rows + 2 * DEPTH
    sds = jax.ShapeDtypeStruct
    reg = (8, cols)
    out, obs = pl.pallas_call(
        functools.partial(model_kernel, mesh.shape["gy"]),
        out_shape=[sds((members * rows, cols), F32), sds((members, cols), F32)],
        in_specs=[vspec()] * 12,
        out_specs=[vspec()] * 2,
        scratch_shapes=[VM((2, n_rows, 8) + reg, F32), VM((n_rows, 8) + reg, F32), VM((n_rows, 8) + reg, F32),
                        VM((3, 8, n_rows, cols), F32),
                        VM((2, 2, 8, 2) + reg, F32), VM((2, 8, 2) + reg, F32), VM((2, 8, 2) + reg, F32),
                        VM((2, 8, 2) + reg, F32), VM(reg, F32)],
        name="model",
    )(state.reshape(members * rows, cols), qt.reshape(-1, cols), qb.reshape(-1, cols),
      fields.reshape(-1, cols), ft.reshape(-1, cols), fb.reshape(-1, cols), mid, top, bot,
      member_mode.reshape(1, members), theta.T, obs_index)
    return out.reshape(members, rows, cols), obs


def sums_kernel(n_gx, n_gy, n_ens, reduce_here, obs_ref, theta_ref, val_ref, sig_ref, full_ref, c_ref, th_ref,
                obs_all, part, rs, c_own, cs, ens_send, ens_recv, rs_send, rs_recv, cs_send, cs_recv, ag_send, ag_recv):
    gx, gy, ens = lax.axis_index("gx"), lax.axis_index("gy"), lax.axis_index("ens")
    members = obs_ref.shape[0]
    n = n_gx * n_gy
    me = gy * n_gx + gx
    peers = [lax.rem(me + o, n) for o in range(1, n)] if reduce_here else []
    where = [{"gx": lax.rem(p, n_gx), "gy": lax.div(p, n_gx)} for p in peers]
    others = [lax.rem(ens + o, n_ens) for o in range(1, n_ens)]

    barrier = pltpu.get_barrier_semaphore()
    for p in others:
        pl.semaphore_signal(barrier, inc=1, device_id={"ens": p}, device_id_type=MESH)
    for p in where:
        pl.semaphore_signal(barrier, inc=1, device_id=p, device_id_type=MESH)
    pl.semaphore_wait(barrier, len(others) + len(where))

    def rdma(src, dst, send, recv, dev):
        return pltpu.make_async_remote_copy(src_ref=src, dst_ref=dst, send_sem=send, recv_sem=recv,
                                            device_id=dev, device_id_type=MESH)

    mine = pl.ds(pl.multiple_of(ens * members, members), members)
    obs_copies, th_copies = [], []
    for k, p in enumerate(others):
        obs_copies.append(rdma(obs_ref, obs_all.at[mine], ens_send.at[2 * k], ens_recv.at[2 * k], {"ens": p}))
        th_copies.append(rdma(theta_ref, th_ref.at[ens], ens_send.at[2 * k + 1], ens_recv.at[2 * k + 1], {"ens": p}))
    for c in obs_copies + th_copies:
        c.start()
    obs_all[mine, :] = obs_ref[...]
    th_ref[ens] = theta_ref[...]
    for c in obs_copies:
        c.wait()

    x = obs_all[...]
    mean = jnp.mean(x, axis=0, keepdims=True)
    inv = 1.0 / sig_ref[0]
    anom = (x - mean) * inv
    d = jnp.broadcast_to((val_ref[0] - mean) * inv, (8, x.shape[1]))
    nt = (((1,), (1,)), ((), ()))
    total = x.shape[0]
    c_part = lax.dot_general(d, anom, nt, preferred_element_type=F32, precision=HIGH)[0:1]
    gram = lax.dot_general(anom, anom, nt, preferred_element_type=F32, precision=HIGH)

    if not reduce_here:
        full_ref[...] = gram
        c_ref[...] = c_part
        for c in th_copies:
            c.wait()
        return
    c_own[...] = c_part
    part[...] = gram
    own = total // n
    at = lambda p: pl.ds(pl.multiple_of(p * own, own), own)
    sends = [rdma(part.at[at(p)], rs.at[k], rs_send.at[k], rs_recv.at[k], w)
             for k, (p, w) in enumerate(zip(peers, where))]
    c_sends = [rdma(c_own, cs.at[k], cs_send.at[k], cs_recv.at[k], w) for k, w in enumerate(where)]
    for c in sends + c_sends:
        c.start()
    acc = part[at(me), :]
    for k, c in enumerate(sends):
        c.wait_recv()
        acc = acc + rs[k]
    full_ref[at(me), :] = acc
    gathers = [rdma(full_ref.at[at(me)], full_ref.at[at(me)], ag_send.at[k], ag_recv.at[k], w)
               for k, w in enumerate(where)]
    for c in gathers:
        c.start()
    acc = c_own[...]
    for k, c in enumerate(c_sends):
        c.wait_recv()
        acc = acc + cs[k]
    c_ref[...] = acc
    for c in sends + c_sends:
        c.wait_send()
    for c in th_copies + gathers:
        c.wait()


def ensemble_sums(mesh, obs, theta, values, sigma):
    n_gx, n_gy, n_ens = mesh.shape["gx"], mesh.shape["gy"], mesh.shape["ens"]
    members, cols = obs.shape
    total = members * n_ens
    n = n_gx * n_gy
    reduce_here = total % (8 * n) == 0
    own = total // n if reduce_here else 8
    slots = n - 1 if reduce_here else 1
    sds = jax.ShapeDtypeStruct
    full, c, th = pl.pallas_call(
        functools.partial(sums_kernel, n_gx, n_gy, n_ens, reduce_here),
        out_shape=[sds((total, total), F32), sds((1, total), F32), sds((n_ens,) + theta.shape[::-1], F32)],
        in_specs=[vspec()] * 4,
        out_specs=[vspec()] * 3,
        scratch_shapes=[VM((total, cols), F32), VM((total, total), F32), VM((slots, own, total), F32),
                        VM((1, total), F32), VM((slots, 1, total), F32)]
        + [pltpu.SemaphoreType.DMA((2 * (n_ens - 1),))] * 2
        + [pltpu.SemaphoreType.DMA((slots,))] * 6,
        compiler_params=pltpu.CompilerParams(collective_id=1, has_side_effects=True),
        name="sums",
    )(obs, theta.T, values, sigma)
    if not reduce_here:
        full, c = lax.psum((full, c), ("gx", "gy"))
    return full, c, th


def solve_kernel(members, full_ref, c_ref, th_ref, out_ref, xs):
    total = full_ref.shape[0]
    blocks = total // 8
    n_ens, params = th_ref.shape[0], th_ref.shape[1]
    shape = (8, total)
    lane = lax.broadcasted_iota(jnp.int32, shape, 1)
    sub = lax.broadcasted_iota(jnp.int32, shape, 0)
    tht = jnp.concatenate([th_ref[e] for e in range(n_ens)], axis=1)
    spread = tht - jnp.mean(tht, axis=1, keepdims=True)
    xs[...] = jnp.zeros_like(xs)
    xs[0:params, :] = spread
    cols_of = xs[...].T
    A, R = [], []
    for k in range(blocks):
        rows = slice(8 * k, 8 * k + 8)
        A.append(full_ref[rows, :] + jnp.where(lane == sub + 8 * k, float(total - 1), 0.0))
        R.append(cols_of[rows])

    def splat(x):
        return jnp.broadcast_to(x, shape)

    for k in range(blocks):
        rs_, rr = [], []
        d = {}
        for j in range(8):
            row = splat(A[k][j:j + 1])
            rs_.append(row)
            rr.append(splat(R[k][j:j + 1]))
            for i in range(j, 8):
                d[j, i] = splat(row[:, 8 * k + i:8 * k + i + 1])
        inv = []
        for j in range(8):
            inv.append(1.0 / d[j, j])
            for i in range(j + 1, 8):
                m = d[j, i] * inv[j]
                rs_[i] = rs_[i] - m * rs_[j]
                rr[i] = rr[i] - m * rr[j]
                for q in range(i, 8):
                    d[i, q] = d[i, q] - m * d[j, q]
        for i in reversed(range(8)):
            for j in range(i + 1, 8):
                rs_[i] = rs_[i] - d[i, j] * rs_[j]
                rr[i] = rr[i] - d[i, j] * rr[j]
            rs_[i] = rs_[i] * inv[i]
            rr[i] = rr[i] * inv[i]
        a, r = rs_[7], rr[7]
        for j in range(7):
            a = jnp.where(sub == j, rs_[j], a)
            r = jnp.where(sub == j, rr[j], r)
        A[k], R[k] = a, r
        for i in list(range(k + 1, blocks)) + list(range(k)):
            a, r = A[i], R[i]
            for j in range(8):
                c = splat(A[i][:, 8 * k + j:8 * k + j + 1])
                if k + 1 < blocks:
                    a = a - c * rs_[j]
                r = r - c * rr[j]
            A[i], R[i] = a, r
    for k in range(blocks):
        xs[8 * k:8 * k + 8, :] = R[k]
    x = xs[...].T[0:8]
    shift = jnp.sum(x * c_ref[...], axis=1, keepdims=True)
    new = (jnp.mean(tht, axis=1, keepdims=True) + shift[0:params]) + float(total - 1) * x[0:params]
    ens = lax.axis_index("ens")
    for e in range(n_ens):
        @pl.when(ens == e)
        def _():
            out_ref[...] = new[:, e * members:(e + 1) * members]


def solve(full, c, th, theta):
    return pl.pallas_call(
        functools.partial(solve_kernel, theta.shape[0]),
        out_shape=jax.ShapeDtypeStruct(theta.shape[::-1], F32),
        in_specs=[vspec()] * 3,
        out_specs=vspec(),
        scratch_shapes=[VM(full.shape, F32)],
        name="solve",
    )(full, c, th).T


def local(mesh, state, u_vel, v_vel, land, forcing, member_mode, theta, obs_index, obs_values, obs_sigma):
    fields, *halos = halo_exchange(mesh, state, forcing, u_vel, v_vel, land)
    final, obs = run_model(mesh, state, fields, halos, member_mode, theta, obs_index)
    full, c, th = ensemble_sums(mesh, obs, theta, obs_values, obs_sigma)
    return final, solve(full, c, th, theta)


def solution(mesh):
    placed = (
        P("ens", "gy", "gx"),
        P("gy", "gx"),
        P("gy", "gx"),
        P("gy", "gx"),
        P(None, "gy", "gx"),
        P("ens"),
        P("ens", None),
        P("gy", "gx", None),
        P("gy", "gx", None),
        P("gy", "gx", None),
    )
    return jax.shard_map(
        functools.partial(local, mesh),
        mesh=mesh,
        in_specs=placed,
        out_specs=(P("ens", "gy", "gx"), P("ens", None)),
        check_vma=False,
    )
```
